32 devices in a mesh: rep: 2 (over y), seq: 4 (over z), head: 2 (over x), sub: 2 (over core).
Axes of the slice: x: 2, y: 2, z: 4, core: 2. Of those that a mesh axis runs over, the one named last changes fastest.
Arguments:
- tokens: bfloat16 [32, 4096], P(('rep', 'sub'), 'seq'), parts along dimension 0, may hold values from -260 to 260
- attn_gain: float32 [4096], P('seq'), may hold values from 0.1 to 1.9
- w_query: bfloat16 [4096, 4096], P('seq', 'head'), may hold values from -0.09375 to 0.09375
- key_projection_weight: bfloat16 [4096, 1024], P('seq', 'head'), may hold values from -0.375 to 0.375
- value_projection_weight: bfloat16 [4096, 1024], P('seq', 'head'), may hold values from -0.375 to 0.375
- w_attn_out: bfloat16 [4096, 4096], P('head', 'seq'), may hold values from -0.09375 to 0.09375
- cache_keys: bfloat16 [32, 8, 2048, 128], P(('rep', 'sub'), 'head', 'seq'), parts along dimension 0, may hold values from -2500 to 2500
- stored_value_cache: bfloat16 [32, 8, 2048, 128], P(('rep', 'sub'), 'head', 'seq'), parts along dimension 0, may hold values from -12 to 12
- lengths: int32 [32], P(('rep', 'sub')), parts along dimension 0, may hold values from 1024 to 2048
- positions: int32 [32], P(('rep', 'sub')), parts along dimension 0, may hold values from 0 to 2047
- mamba_gain: float32 [4096], replicated, may hold values from 0.1 to 1.9
- w_in: bfloat16 [2, 4096, 8192], P(None, None, ('seq', 'head')), may hold values from -0.09375 to 0.09375
- conv_weight: float32 [4, 8192], P(None, ('seq', 'head')), may hold values from -3 to 3
- conv_bias: float32 [8192], P(('seq', 'head')), may hold values from -0.5 to 0.5
- conv_state: float32 [32, 3, 8192], P(('rep', 'sub'), None, ('seq', 'head')), parts along dimension 0, may hold values from -6 to 6
- w_xproj: bfloat16 [8192, 288], P(('seq', 'head')), may hold values from -0.0625 to 0.0625
- w_dt: bfloat16 [256, 8192], P(None, ('seq', 'head')), may hold values from -0.375 to 0.375
- dt_bias: float32 [8192], P(('seq', 'head')), may hold values from -4 to 0
- a_log: float32 [16, 8192], P(None, ('seq', 'head')), may hold values from 0 to 2.77
- skip_gain: float32 [8192], P(('seq', 'head')), may hold values from 0.25 to 2
- ssm_state: float32 [32, 16, 8192], P(('rep', 'sub'), None, ('seq', 'head')), parts along dimension 0, may hold values from -6 to 6
- w_mamba_out: bfloat16 [8192, 4096], P(('seq', 'head')), may hold values from -0.09375 to 0.09375
Outputs:
- hidden_out: bfloat16 [32, 4096], P(('rep', 'sub'), 'seq'), parts along dimension 0
- new_state: float32 [32, 16, 8192], P(('rep', 'sub'), None, ('seq', 'head')), parts along dimension 0
The draws below stay inside these ranges and needn't reach their ends.
There are 2 independent parts, one for each index of `rep`. The reference program is written for one: setup_inputs(seed, part) draws one part's arguments, and reference() takes and returns one part's arrays. A program takes and returns all parts, laid end to end along the dimension named above; an argument that names none is the same for every part. Nothing has to cross between parts.
Inputs may be any that keep to these rules, and one draw needn't show every extreme that they name: Cache positions p < lengths[b] hold sequence b's past keys and values; later positions are not attended.
All inputs are finite; a program needn't handle non-finite values.
Results may differ from the reference program's by a relative error of at most 0.015.
Values may be sent and summed in bfloat16 or wider, within the bound.
No kernel may reach another device: no remote copies, remote signals or barrier semaphores. Data moves between devices by JAX's collectives and lax.ppermute only.
A program may use at most 128 MiB of HBM per device.

```python
import math
import jax
import jax.numpy as jnp
from jax import lax

MODEL_DIMENSION = 4096
QUERY_HEADS = 32
KEY_VALUE_HEADS = 8
HEAD_SIZE = 128
DI = 8192
NSTATE = 16
DT_RANK = 256
KCONV = 4
BATCH_SEQUENCES = 16
CACHE_POSITIONS = 2048


def draw_tokens(key, part):
    base_key_rows = jax.random.fold_in(jax.random.fold_in(key, 11), 0)
    base_draw = jnp.clip(jax.random.normal(base_key_rows, (BATCH_SEQUENCES, MODEL_DIMENSION), jnp.float32), -6.0, 6.0)
    across = jnp.arange(MODEL_DIMENSION, dtype=jnp.float32) / MODEL_DIMENSION
    value_vectors = base_draw * jnp.sqrt(1.0 + 2.0 * across)[None, :]
    return value_vectors.astype(jnp.bfloat16)


def draw_cache_keys(key, part):
    base_key_rows = jax.random.fold_in(jax.random.fold_in(key, 23), 0)
    value_vectors = 2.5 * jnp.clip(jax.random.normal(base_key_rows, (BATCH_SEQUENCES, KEY_VALUE_HEADS, CACHE_POSITIONS, HEAD_SIZE), jnp.float32), -6.0, 6.0)
    return value_vectors.astype(jnp.bfloat16)


def draw_stored_value_cache(key, part):
    noise_key, common_key = jax.random.split(jax.random.fold_in(key, 37), 2)
    shape = (BATCH_SEQUENCES, KEY_VALUE_HEADS, CACHE_POSITIONS, HEAD_SIZE)
    common = jnp.clip(jax.random.normal(common_key, (BATCH_SEQUENCES, KEY_VALUE_HEADS, 1, HEAD_SIZE), jnp.float32), -4.0, 4.0)
    along = (jnp.arange(CACHE_POSITIONS, dtype=jnp.float32) / CACHE_POSITIONS)[None, None, :, None]
    noise = jnp.clip(jax.random.normal(noise_key, shape, jnp.float32), -6.0, 6.0)
    ramp = 0.3 + 0.7 * along
    return (noise + ramp * common).astype(jnp.bfloat16)


def set_ends(result, own_key, least, largest):
    dims = result.shape
    spot = [jax.random.randint(jax.random.fold_in(own_key, axis), (), 0, dims[axis]) for axis in range(len(dims))]
    result = result.at[tuple(spot)].set(least)
    longest = dims.index(max(dims))
    spot[longest] = (spot[longest] + 1) % dims[longest]
    return result.at[tuple(spot)].set(largest)


def raised(result, stream_key, source, target, shards_of, factor):
    owner, partner = [(jnp.arange(result.shape[dim]) // (result.shape[dim] // shards_of)).reshape([-1 if axis == dim else 1 for axis in range(result.ndim)]) for dim in (source, target)]
    chosen = jax.random.permutation(stream_key, shards_of)[partner]
    strong = (owner == chosen) | (owner == (partner + shards_of // 2) % shards_of)
    return jnp.where(strong, factor * result, result)


def shard_levels(stream_key, dims, shards, least, largest):
    level = 1.0
    for dim, blocks in shards:
        heights = jax.random.uniform(jax.random.fold_in(jax.random.fold_in(stream_key, 6), dim), (blocks,), jnp.float32, least / len(shards), largest / len(shards))
        level = level * jnp.repeat(jnp.exp(heights), dims[dim] // blocks).reshape((-1,) + (1,) * (len(dims) - 1 - dim))
    return level


def normal_values(own_key, extent, deviation, reach, pieces=(), held_as=jnp.bfloat16):
    array = deviation * jax.random.normal(own_key, extent, jnp.float32)
    if pieces:
        array = array * shard_levels(own_key, extent, pieces, -0.22, 0.18)
    return jnp.clip(array, -reach, reach).astype(held_as)


def bell_draw_with(own_key, shape, spread, most, pieces, heavy, kind=jnp.bfloat16):
    drawn = spread * jax.random.normal(own_key, shape, jnp.float32)
    if pieces:
        drawn = drawn * shard_levels(own_key, shape, pieces, -0.22, 0.18)
    return jnp.clip(raised(drawn, jax.random.fold_in(own_key, 3), *heavy), -most, most).astype(kind)


def setup_inputs(seed: int = 0, part: int = 0) -> dict:
    keys = jax.random.split(jax.random.key(seed), 23)
    own_keys = jax.random.split(jax.random.fold_in(keys[22], part), 23)
    tokens = draw_tokens(jax.random.fold_in(jax.random.fold_in(keys[22], part), 71), part)
    attn_gain = jnp.clip(1.0 + 0.18 * jax.random.normal(keys[1], (MODEL_DIMENSION,), jnp.float32), 0.1, 1.9)
    w_query = normal_values(keys[2], (MODEL_DIMENSION, QUERY_HEADS * HEAD_SIZE), MODEL_DIMENSION ** -0.5, 0.09375, ((0, 4), (1, 2)))
    key_projection_weight = normal_values(keys[3], (MODEL_DIMENSION, KEY_VALUE_HEADS * HEAD_SIZE), (MODEL_DIMENSION // 16) ** -0.5, 0.375, ((0, 4), (1, 2)))
    value_projection_weight = normal_values(keys[4], (MODEL_DIMENSION, KEY_VALUE_HEADS * HEAD_SIZE), (MODEL_DIMENSION // 16) ** -0.5, 0.375, ((0, 4), (1, 2)))
    w_attn_out = normal_values(keys[5], (QUERY_HEADS * HEAD_SIZE, MODEL_DIMENSION), (QUERY_HEADS * HEAD_SIZE) ** -0.5, 0.09375, ((0, 2), (1, 4)))
    cache_keys = draw_cache_keys(jax.random.fold_in(jax.random.fold_in(keys[22], part), 71), part)
    stored_value_cache = draw_stored_value_cache(jax.random.fold_in(jax.random.fold_in(keys[22], part), 71), part)
    lengths = set_ends(jax.random.randint(own_keys[8], (BATCH_SEQUENCES,), CACHE_POSITIONS // 2, CACHE_POSITIONS + 1), jax.random.fold_in(own_keys[8], 1), CACHE_POSITIONS // 2, CACHE_POSITIONS).astype(jnp.int32)
    positions = set_ends(jax.random.randint(own_keys[9], (BATCH_SEQUENCES,), 0, CACHE_POSITIONS), jax.random.fold_in(own_keys[9], 1), 0, CACHE_POSITIONS - 1).astype(jnp.int32)
    mamba_gain = jnp.clip(1.0 + 0.18 * jax.random.normal(keys[10], (MODEL_DIMENSION,), jnp.float32), 0.1, 1.9)
    w_in = normal_values(keys[11], (2, MODEL_DIMENSION, DI), MODEL_DIMENSION ** -0.5, 0.09375, ((2, 8),))
    conv_weight = normal_values(keys[12], (KCONV, DI), KCONV ** -0.5, 3.0, ((1, 8),), jnp.float32)
    conv_bias = jnp.clip(jax.random.uniform(keys[13], (DI,), jnp.float32, -0.5, 0.5) * shard_levels(keys[13], (DI,), ((0, 8),), -0.4, 0.0), -0.5, 0.5)
    conv_state = normal_values(own_keys[14], (BATCH_SEQUENCES, KCONV - 1, DI), 1.0, 6.0, ((0, 2), (2, 8)), jnp.float32)
    w_xproj = normal_values(keys[15], (DI, DT_RANK + 2 * NSTATE), DI ** -0.5, 0.0625, ((0, 8),))
    w_dt = normal_values(keys[16], (DT_RANK, DI), DT_RANK ** -0.5, 0.375, ((1, 8),))
    dt_bias = jnp.clip(-4.0 + 4.0 * jax.random.uniform(keys[17], (DI,), jnp.float32) ** shard_levels(keys[17], (DI,), ((0, 8),), -0.2, 0.2), -4.0, 0.0)
    a_log = jnp.clip(2.77 * jax.random.uniform(keys[18], (NSTATE, DI), jnp.float32) ** shard_levels(keys[18], (NSTATE, DI), ((1, 8),), -0.2, 0.2), 0.0, 2.77)
    skip_gain = jnp.clip(0.25 + 1.75 * jax.random.uniform(keys[19], (DI,), jnp.float32) ** shard_levels(keys[19], (DI,), ((0, 8),), -0.2, 0.2), 0.25, 2.0)
    ssm_state = normal_values(own_keys[20], (BATCH_SEQUENCES, NSTATE, DI), 1.0, 6.0, ((0, 2), (2, 8)), jnp.float32)
    w_mamba_out = bell_draw_with(keys[21], (DI, MODEL_DIMENSION), DI ** -0.5, 0.09375, ((0, 8),), (0, 1, 8, 2.0))
    return {"tokens": tokens, "attn_gain": attn_gain, "w_query": w_query, "key_projection_weight": key_projection_weight, "value_projection_weight": value_projection_weight, "w_attn_out": w_attn_out, "cache_keys": cache_keys, "stored_value_cache": stored_value_cache, "lengths": lengths, "positions": positions, "mamba_gain": mamba_gain, "w_in": w_in, "conv_weight": conv_weight, "conv_bias": conv_bias, "conv_state": conv_state, "w_xproj": w_xproj, "w_dt": w_dt, "dt_bias": dt_bias, "a_log": a_log, "skip_gain": skip_gain, "ssm_state": ssm_state, "w_mamba_out": w_mamba_out}


norm_eps = 1e-05
rope_base = 10000.0

def apply_rotary(vectors, positions):
    half_dim = vectors.shape[-1] // 2
    frequency = jnp.exp(-math.log(rope_base) * 2.0 * jnp.arange(half_dim, dtype=jnp.float32) / (2 * half_dim))
    angles = positions.astype(jnp.float32)[:, None] * frequency[None, :]
    cosine = jnp.cos(angles)[:, None, :]
    sine_part = jnp.sin(angles)[:, None, :]
    first_half = vectors[..., :half_dim]
    second_half = vectors[..., half_dim:]
    return jnp.concatenate([first_half * cosine - second_half * sine_part, second_half * cosine + first_half * sine_part], axis=-1)

def reference(tokens, attn_gain, w_query, key_projection_weight, value_projection_weight, w_attn_out, cache_keys, stored_value_cache, lengths, positions, mamba_gain, w_in, conv_weight, conv_bias, conv_state, w_xproj, w_dt, dt_bias, a_log, skip_gain, ssm_state, w_mamba_out):
    token_float = tokens.astype(jnp.float32)
    inv_rms = lax.rsqrt(lax.optimization_barrier(jnp.sum(token_float * token_float, axis=1)) / MODEL_DIMENSION + norm_eps)
    lifted = (token_float * attn_gain[None, :]).astype(jnp.bfloat16)
    query_vectors = jnp.dot(lifted, w_query, preferred_element_type=jnp.float32) * inv_rms[:, None]
    fresh_key_rows = jnp.dot(lifted, key_projection_weight, preferred_element_type=jnp.float32) * inv_rms[:, None]
    fresh_value_rows = jnp.dot(lifted, value_projection_weight, preferred_element_type=jnp.float32) * inv_rms[:, None]
    query_vectors = apply_rotary(query_vectors.reshape(BATCH_SEQUENCES, QUERY_HEADS, HEAD_SIZE), positions).astype(jnp.bfloat16)
    fresh_key_rows = apply_rotary(fresh_key_rows.reshape(BATCH_SEQUENCES, KEY_VALUE_HEADS, HEAD_SIZE), positions).astype(jnp.bfloat16)
    fresh_value_rows = fresh_value_rows.reshape(BATCH_SEQUENCES, KEY_VALUE_HEADS, HEAD_SIZE).astype(jnp.bfloat16)
    query_group_count = QUERY_HEADS // KEY_VALUE_HEADS
    grouped_queries = query_vectors.reshape(BATCH_SEQUENCES, KEY_VALUE_HEADS, query_group_count, HEAD_SIZE).astype(jnp.float32)
    score_scale = HEAD_SIZE ** (-0.5)
    scores = jnp.einsum('bhgd,bhtd->bhgt', grouped_queries, cache_keys.astype(jnp.float32)) * score_scale
    score_new = jnp.einsum('bhgd,bhd->bhg', grouped_queries, fresh_key_rows.astype(jnp.float32)) * score_scale
    live_mask = jnp.arange(CACHE_POSITIONS, dtype=jnp.int32)[None, None, None, :] < lengths[:, None, None, None]
    row_max = jnp.maximum(lax.optimization_barrier(jnp.max(jnp.where(live_mask, scores, -jnp.inf), axis=-1)), score_new)
    weights = jnp.where(live_mask, jnp.exp(scores - row_max[..., None]), 0.0)
    new_weight = jnp.exp(score_new - row_max)
    total_weight = lax.optimization_barrier(jnp.sum(weights, axis=-1)) + new_weight
    rounded = lax.optimization_barrier(weights.astype(jnp.bfloat16)).astype(jnp.float32)
    attended = jnp.einsum('bhgt,bhtd->bhgd', rounded, stored_value_cache.astype(jnp.float32))
    attended = attended + new_weight[..., None] * fresh_value_rows.astype(jnp.float32)[:, :, None, :]
    attn_rows = (attended / total_weight[..., None]).reshape(BATCH_SEQUENCES, QUERY_HEADS * HEAD_SIZE).astype(jnp.bfloat16)
    mid_stream = (token_float + jnp.dot(attn_rows, w_attn_out, preferred_element_type=jnp.float32)).astype(jnp.bfloat16)
    mid_float = mid_stream.astype(jnp.float32)
    inv_rms_two = lax.rsqrt(lax.optimization_barrier(jnp.mean(mid_float * mid_float, axis=1)) + norm_eps)
    lifted_two = (mid_float * inv_rms_two[:, None] * mamba_gain[None, :]).astype(jnp.bfloat16)
    inner = jnp.dot(lifted_two, w_in[0], preferred_element_type=jnp.float32)
    gate_branch = jnp.dot(lifted_two, w_in[1], preferred_element_type=jnp.float32)
    window = jnp.concatenate([conv_state, inner[:, None, :]], axis=1)
    mixed = lax.optimization_barrier(jnp.sum(window * conv_weight[None, :, :], axis=1)) + conv_bias[None, :]
    activated = jax.nn.silu(mixed)
    projected = jnp.dot(activated.astype(jnp.bfloat16), w_xproj, preferred_element_type=jnp.float32)
    dt_low = projected[:, :DT_RANK].astype(jnp.bfloat16)
    input_map = projected[:, DT_RANK:DT_RANK + NSTATE]
    output_map = projected[:, DT_RANK + NSTATE:]
    step_size = jax.nn.softplus(jnp.dot(dt_low, w_dt, preferred_element_type=jnp.float32) + dt_bias[None, :])
    decay = jnp.exp(step_size[:, None, :] * (-jnp.exp(a_log))[None, :, :])
    new_state = decay * ssm_state + (step_size * activated)[:, None, :] * input_map[:, :, None]
    readout = lax.optimization_barrier(jnp.sum(output_map[:, :, None] * new_state, axis=1)) + skip_gain[None, :] * activated
    gated = (readout * jax.nn.silu(gate_branch)).astype(jnp.bfloat16)
    hidden_out = (mid_float + jnp.dot(gated, w_mamba_out, preferred_element_type=jnp.float32)).astype(jnp.bfloat16)
    return (hidden_out, new_state)
```

```python
import math

import jax
import jax.numpy as jnp
from jax import lax
from jax.sharding import PartitionSpec as P


norm_eps = 1e-05
masked_floor = -1e30
rope_base = 10000.0
group_axes = ("seq", "head")


def from_partners(value, axis):
    count = lax.axis_size(axis)
    if count & (count - 1) == 0 and count <= 4:
        return [
            lax.ppermute(value, axis, [(i, i ^ k) for i in range(count)]) for k in range(1, count)
        ]
    return [
        lax.ppermute(value, axis, [(i, (i + k) % count) for i in range(count)])
        for k in range(1, count)
    ]


def from_group(value):
    return lax.all_to_all(value, group_axes, 0, 0, tiled=False)


def rotary_tables(positions, head_dim):
    half_dim = head_dim // 2
    frequency = jnp.exp(
        -math.log(rope_base) * 2.0 * jnp.arange(half_dim, dtype=jnp.float32) / (2 * half_dim)
    )
    angles = positions.astype(jnp.float32)[:, None] * frequency[None, :]
    return jnp.cos(angles), jnp.sin(angles)


def apply_rotary(vectors, cosine, sine_part):
    half_dim = vectors.shape[-1] // 2
    first_half = vectors[..., :half_dim]
    second_half = vectors[..., half_dim:]
    cosine = cosine[:, None, :]
    sine_part = sine_part[:, None, :]
    return jnp.concatenate(
        [
            first_half * cosine - second_half * sine_part,
            second_half * cosine + first_half * sine_part,
        ],
        axis=-1,
    )


def in_three(value):
    high = value.astype(jnp.bfloat16)
    rest = value - high.astype(jnp.float32)
    middle = rest.astype(jnp.bfloat16)
    low = (rest - middle.astype(jnp.float32)).astype(jnp.bfloat16)
    return jnp.concatenate([high, middle, low], axis=-1)


def local(
    tokens,
    attn_gain,
    w_query,
    key_projection_weight,
    value_projection_weight,
    w_attn_out,
    cache_keys,
    stored_value_cache,
    lengths,
    positions,
    mamba_gain,
    w_in,
    conv_weight,
    conv_bias,
    conv_state,
    w_xproj,
    w_dt,
    dt_bias,
    a_log,
    skip_gain,
    ssm_state,
    w_mamba_out,
):
    f32 = jnp.float32
    bf16 = jnp.bfloat16
    rows, cols = tokens.shape
    head_dim = cache_keys.shape[3]
    kv_local = cache_keys.shape[1]
    ctx_local = cache_keys.shape[2]
    q_width = w_query.shape[1]
    kv_width = kv_local * head_dim
    q_local = q_width // head_dim
    per_kv = q_local // kv_local
    seq_size = lax.axis_size("seq")
    head_size = lax.axis_size("head")
    group = seq_size * head_size
    width = cols * seq_size

    token_float = tokens.astype(f32)
    lifted = (token_float * attn_gain[None, :]).astype(bf16)
    part = jnp.concatenate(
        [
            jnp.dot(lifted, w_query, preferred_element_type=f32),
            jnp.dot(lifted, key_projection_weight, preferred_element_type=f32),
            jnp.dot(lifted, value_projection_weight, preferred_element_type=f32),
        ],
        axis=1,
    )
    squares = jnp.sum(token_float * token_float, axis=1, keepdims=True)
    sent = jnp.concatenate(
        [part.astype(bf16), jnp.pad(in_three(squares), ((0, 0), (0, 125)))], axis=1
    )
    total_width = part.shape[1]
    for other in from_partners(sent, "seq"):
        part = part + other[:, :total_width].astype(f32)
        squares = squares + jnp.sum(
            other[:, total_width:].astype(f32), axis=1, keepdims=True
        )
    inv_rms = lax.rsqrt(squares / width + norm_eps)
    part = part * inv_rms
    cosine, sine_part = rotary_tables(positions, head_dim)
    query = apply_rotary(
        part[:, :q_width].reshape(rows, q_local, head_dim), cosine, sine_part
    ).astype(bf16)
    key_new = apply_rotary(
        part[:, q_width : q_width + kv_width].reshape(rows, kv_local, head_dim), cosine, sine_part
    ).astype(bf16)
    value_new = part[:, q_width + kv_width :].reshape(rows, kv_local, head_dim).astype(bf16)

    grouped = query.reshape(rows, kv_local, per_kv, head_dim)
    score_scale = head_dim ** (-0.5)
    scores = (
        jnp.einsum("bhgd,bhtd->bhgt", grouped, cache_keys, preferred_element_type=f32)
        * score_scale
    )
    slot = lax.axis_index("seq") * ctx_local + jnp.arange(ctx_local, dtype=jnp.int32)
    live = slot[None, None, None, :] < lengths[:, None, None, None]
    local_max = jnp.max(jnp.where(live, scores, masked_floor), axis=-1)
    weights = jnp.where(live, jnp.exp(scores - local_max[..., None]), 0.0)
    local_sum = jnp.sum(weights, axis=-1)
    local_acc = jnp.einsum(
        "bhgt,bhtd->bhgd", weights.astype(bf16), stored_value_cache, preferred_element_type=f32
    )
    some = local_sum > 0.0
    safe_sum = jnp.where(some, local_sum, 1.0)
    level = jnp.where(some, local_max + jnp.log(safe_sum), masked_floor).reshape(rows, q_local)
    mean = (local_acc / safe_sum[..., None]).reshape(rows, q_width)
    pad = (-3 * q_local) % 128
    sent = jnp.concatenate(
        [mean.astype(bf16), jnp.pad(in_three(level), ((0, 0), (0, pad)))], axis=1
    )
    means = [mean]
    levels = [level]
    for other in from_partners(sent, "seq"):
        means.append(other[:, :q_width].astype(f32))
        terms = other[:, q_width : q_width + 3 * q_local].astype(f32)
        levels.append(
            (terms[:, :q_local] + terms[:, q_local : 2 * q_local]) + terms[:, 2 * q_local :]
        )
    score_new = (
        jnp.sum(grouped.astype(f32) * key_new.astype(f32)[:, :, None, :], axis=-1) * score_scale
    ).reshape(rows, q_local)
    levels.append(score_new)
    means.append(
        jnp.broadcast_to(
            value_new.astype(f32)[:, :, None, :], (rows, kv_local, per_kv, head_dim)
        ).reshape(rows, q_width)
    )
    top = levels[0]
    for level in levels[1:]:
        top = jnp.maximum(top, level)
    factors = [jnp.exp(level - top) for level in levels]
    total = sum(factors[1:], factors[0])
    attended = 0.0
    for factor, mean in zip(factors, means):
        attended = attended + (factor / total)[:, :, None] * mean.reshape(
            rows, q_local, head_dim
        )
    attn_rows = attended.reshape(rows, q_width).astype(bf16)

    out_part = jnp.dot(attn_rows, w_attn_out, preferred_element_type=f32)
    first = lax.axis_index("head") == 0
    out_part = (out_part + jnp.where(first, token_float, 0.0)).astype(bf16)
    pieces = from_group(jnp.broadcast_to(out_part[None], (group, rows, cols)))
    pieces = pieces.reshape(seq_size, head_size, rows, cols).astype(f32)
    mid_blocks = jnp.sum(pieces, axis=1)
    mid_own = lax.dynamic_index_in_dim(mid_blocks, lax.axis_index("seq"), 0, keepdims=False)
    mid = jnp.concatenate([mid_blocks[i] for i in range(seq_size)], axis=1)
    inv_rms_two = lax.rsqrt(jnp.mean(mid * mid, axis=1) + norm_eps)
    lifted_two = (mid * inv_rms_two[:, None] * mamba_gain[None, :]).astype(bf16)
    inner = jnp.dot(lifted_two, w_in[0], preferred_element_type=f32)
    gate_branch = jnp.dot(lifted_two, w_in[1], preferred_element_type=f32)
    taps = conv_state.shape[1]
    mixed = inner * conv_weight[taps][None, :] + conv_bias[None, :]
    for k in range(taps):
        mixed = mixed + conv_state[:, k, :] * conv_weight[k][None, :]
    activated = jax.nn.silu(mixed)
    proj_part = jnp.dot(activated.astype(bf16), w_xproj, preferred_element_type=f32)
    projected = jnp.sum(
        from_group(jnp.broadcast_to(proj_part[None], (group,) + proj_part.shape)), axis=0
    )
    rank_width = w_dt.shape[0]
    state_width = ssm_state.shape[1]
    dt_low = projected[:, :rank_width].astype(bf16)
    input_map = projected[:, rank_width : rank_width + state_width]
    output_map = projected[:, rank_width + state_width :]
    step_size = jax.nn.softplus(
        jnp.dot(dt_low, w_dt, preferred_element_type=f32) + dt_bias[None, :]
    )
    decay = jnp.exp(step_size[:, None, :] * (-jnp.exp(a_log))[None, :, :])
    new_state = decay * ssm_state + (step_size * activated)[:, None, :] * input_map[:, :, None]
    readout = jnp.sum(output_map[:, :, None] * new_state, axis=1) + skip_gain[None, :] * activated
    gated = (readout * jax.nn.silu(gate_branch)).astype(bf16)
    mamba_part = jnp.dot(gated, w_mamba_out, preferred_element_type=f32).astype(bf16)
    blocks = [
        mamba_part[:, i * cols : (i + 1) * cols] for i in range(seq_size) for _ in range(head_size)
    ]
    share = jnp.sum(from_group(jnp.stack(blocks)).astype(f32), axis=0)
    hidden_out = (mid_own + share).astype(bf16)
    return (hidden_out, new_state)


def solution(mesh):
    in_specs = (
        P(("rep", "sub"), "seq"),
        P("seq"),
        P("seq", "head"),
        P("seq", "head"),
        P("seq", "head"),
        P("head", "seq"),
        P(("rep", "sub"), "head", "seq", None),
        P(("rep", "sub"), "head", "seq", None),
        P(("rep", "sub")),
        P(("rep", "sub")),
        P(),
        P(None, None, ("seq", "head")),
        P(None, ("seq", "head")),
        P(("seq", "head")),
        P(("rep", "sub"), None, ("seq", "head")),
        P(("seq", "head"), None),
        P(None, ("seq", "head")),
        P(("seq", "head")),
        P(None, ("seq", "head")),
        P(("seq", "head")),
        P(("rep", "sub"), None, ("seq", "head")),
        P(("seq", "head"), None),
    )
    out_specs = (P(("rep", "sub"), "seq"), P(("rep", "sub"), None, ("seq", "head")))
    return jax.shard_map(local, mesh=mesh, in_specs=in_specs, out_specs=out_specs, check_vma=False)
```

```python
import functools
import math

import jax
import jax.numpy as jnp
from jax import lax
from jax.experimental import pallas as pl
from jax.experimental.pallas import tpu as pltpu
from jax.sharding import PartitionSpec as P


norm_eps = 1e-05
masked_floor = -1e30
rope_base = 10000.0
group_axes = ("seq", "head")


def from_partners(value, axis):
    count = lax.axis_size(axis)
    if count & (count - 1) == 0 and count <= 4:
        return [
            lax.ppermute(value, axis, [(i, i ^ k) for i in range(count)]) for k in range(1, count)
        ]
    return [
        lax.ppermute(value, axis, [(i, (i + k) % count) for i in range(count)])
        for k in range(1, count)
    ]


def from_group(value):
    return lax.all_to_all(value, group_axes, 0, 0, tiled=False)


f32 = jnp.float32
bf16 = jnp.bfloat16
LANES = 128
WEIGHT = 10**12
in_vmem = pl.BlockSpec(memory_space=pltpu.VMEM)
in_smem = pl.BlockSpec(memory_space=pltpu.SMEM)
in_any = pl.BlockSpec(memory_space=pl.ANY)


def far(value):
    return pltpu.with_memory_space_constraint(value, pltpu.HBM)


def call(kernel, out_shape, operands, name, limit, flops, scratch=(), spaces=None):
    size = sum(math.prod(x.shape) * x.dtype.itemsize for x in operands)
    return pl.pallas_call(
        kernel,
        out_shape=out_shape,
        in_specs=spaces or [in_vmem] * len(operands),
        out_specs=jax.tree.map(lambda _: in_vmem, out_shape),
        scratch_shapes=scratch,
        name=name,
        cost_estimate=pl.CostEstimate(flops=WEIGHT, bytes_accessed=size, transcendentals=0),
        compiler_params=pltpu.CompilerParams(vmem_limit_bytes=limit),
    )(*operands)


def column(ref, rows):
    row = lax.broadcasted_iota(jnp.int32, (rows, LANES), 0)
    result = jnp.zeros((rows, LANES), jnp.int32)
    for b in range(rows):
        result = jnp.where(row == b, ref[b], result)
    return result


def in_three(value):
    high = value.astype(bf16).astype(f32)
    rest = value - high
    middle = rest.astype(bf16).astype(f32)
    return high, middle, rest - middle


def project_kernel(
    chunks, tok, gain, positions, wq, wk, wv, sent, part, square, cosine, sine, *scratch
):
    wq_buf, wk_buf, wv_buf, sems = scratch
    rows, cols = tok.shape
    depth = cols // chunks
    copies = []
    for c in range(chunks):
        span = pl.ds(c * depth, depth)
        for i, (source, target) in enumerate(((wq, wq_buf), (wk, wk_buf), (wv, wv_buf))):
            copy = pltpu.make_async_copy(source.at[span], target.at[span], sems.at[i, c])
            copy.start()
            copies.append(copy)
    value = tok[...].astype(f32)
    lifted = (value * gain[...]).astype(bf16)
    squares = jnp.sum(value * value, axis=1, keepdims=True)
    lane = lax.broadcasted_iota(jnp.int32, (rows, LANES), 1)
    half = cosine.shape[1] // 2
    frequency = jnp.exp(-math.log(rope_base) / half * lax.rem(lane, half).astype(f32))
    angles = column(positions, rows).astype(f32) * frequency
    cosine[...] = jnp.cos(angles)
    sine[...] = jnp.where(lane < half, -1.0, 1.0) * jnp.sin(angles)
    sums = [0.0, 0.0, 0.0]
    for c in range(chunks):
        x = lifted[:, c * depth : (c + 1) * depth]
        for i, buf in enumerate((wq_buf, wk_buf, wv_buf)):
            copies[3 * c + i].wait()
            sums[i] = sums[i] + jnp.dot(
                x, buf[c * depth : (c + 1) * depth], preferred_element_type=f32
            )
    start = 0
    for total in sums:
        stop = start + total.shape[1]
        part[:, start:stop] = total
        sent[:, start:stop] = total.astype(bf16)
        start = stop
    high, middle, low = in_three(squares)
    terms = jnp.where(lane == 0, high, jnp.where(lane == 1, middle, jnp.where(lane == 2, low, 0.0)))
    sent[:, start : start + LANES] = terms.astype(bf16)
    square[...] = jnp.broadcast_to(squares, (rows, LANES))


def attend_kernel(width, count, *refs):
    part, square = refs[0], refs[1]
    others = refs[2 : 1 + count]
    cosine, sine, lengths, keys, values = refs[1 + count : 6 + count]
    sent, mean_out, level_out, score_out, value_out = refs[6 + count :]
    rows, total_width = part.shape
    kv_heads, depth, head_dim = keys.shape[1:]
    kv_width = kv_heads * head_dim
    q_width = total_width - 2 * kv_width
    heads = q_width // head_dim
    per_kv = heads // kv_heads
    scale = head_dim ** (-0.5)
    squares = square[...]
    for other in others:
        terms = other[:, total_width : total_width + LANES].astype(f32)
        squares = squares + jnp.sum(terms, axis=1, keepdims=True)
    inv_rms = lax.rsqrt(squares / width + norm_eps)

    def summed(start):
        total = part[:, start : start + head_dim]
        for other in others:
            total = total + other[:, start : start + head_dim].astype(f32)
        return total * inv_rms

    def rotated(start):
        x = summed(start)
        x = x * cosine[...] + pltpu.roll(x, head_dim // 2, 1) * sine[...]
        return x.astype(bf16).astype(f32)

    tall = per_kv * rows
    owner = lax.rem(lax.broadcasted_iota(jnp.int32, (tall, depth), 0), rows)
    slot = lax.broadcasted_iota(jnp.int32, (tall, depth), 1)
    limit = column(lengths, rows)[:, :1] - lax.axis_index("seq") * depth
    live = slot < jnp.concatenate([limit] * per_kv, axis=0)
    lane = lax.broadcasted_iota(jnp.int32, (rows, LANES), 1)
    levels = jnp.zeros((rows, LANES), f32)
    fresh = jnp.zeros((rows, LANES), f32)
    for h in range(kv_heads):
        queries = [rotated((h * per_kv + j) * head_dim) for j in range(per_kv)]
        key_new = rotated(q_width + h * head_dim)
        value_new = summed(q_width + kv_width + h * head_dim).astype(bf16).astype(f32)
        value_out[:, h * head_dim : (h + 1) * head_dim] = value_new
        for j in range(per_kv):
            score = jnp.sum(queries[j] * key_new, axis=1, keepdims=True) * scale
            fresh = jnp.where(lane == h * per_kv + j, score, fresh)
        stacked = jnp.concatenate(queries, axis=0).astype(bf16)
        scores = jnp.zeros((tall, depth), f32)
        for b in range(rows):
            mine = lax.dot_general(
                stacked, keys[b, h], (((1,), (1,)), ((), ())), preferred_element_type=f32
            )
            scores = jnp.where(owner == b, mine, scores)
        scores = jnp.where(live, scores * scale, masked_floor)
        top = jnp.max(scores, axis=1, keepdims=True)
        weights = jnp.where(live, jnp.exp(scores - top), 0.0)
        total = jnp.sum(weights, axis=1, keepdims=True)
        acc = jnp.zeros((tall, head_dim), f32)
        for b in range(rows):
            mine = jnp.where(owner == b, weights, 0.0).astype(bf16)
            acc = acc + jnp.dot(mine, values[b, h], preferred_element_type=f32)
        some = total > 0.0
        safe = jnp.where(some, total, 1.0)
        level = jnp.where(some, top + jnp.log(safe), masked_floor)
        acc = acc / safe
        for j in range(per_kv):
            head = h * per_kv + j
            block = acc[j * rows : (j + 1) * rows]
            mean_out[:, head * head_dim : (head + 1) * head_dim] = block
            sent[:, head * head_dim : (head + 1) * head_dim] = block.astype(bf16)
            levels = jnp.where(lane == head, level[j * rows : (j + 1) * rows], levels)
    level_out[...] = levels
    score_out[...] = fresh
    high, middle, low = in_three(levels)
    packed = high + pltpu.roll(middle, heads, 1) + pltpu.roll(low, 2 * heads, 1)
    sent[:, q_width : q_width + LANES] = packed.astype(bf16)


def merge_kernel(heads, count, *refs):
    mean, level = refs[0], refs[1]
    others = refs[2 : 1 + count]
    score_new, value_new, tok, w_out, out = refs[1 + count :]
    rows, q_width = mean.shape
    head_dim = q_width // heads
    per_kv = q_width // value_new.shape[1]
    levels = [level[...]]
    for other in others:
        packed = other[:, q_width : q_width + LANES].astype(f32)
        levels.append(
            (packed + pltpu.roll(packed, LANES - heads, 1))
            + pltpu.roll(packed, LANES - 2 * heads, 1)
        )
    levels.append(score_new[...])
    top = functools.reduce(jnp.maximum, levels)
    factors = [jnp.exp(x - top) for x in levels]
    total = functools.reduce(jnp.add, factors)
    factors = [x / total for x in factors]
    blocks = []
    for j in range(heads):
        span = slice(j * head_dim, (j + 1) * head_dim)
        kv = j // per_kv
        terms = [mean[:, span]] + [other[:, span].astype(f32) for other in others]
        terms.append(value_new[:, kv * head_dim : (kv + 1) * head_dim])
        block = 0.0
        for factor, term in zip(factors, terms):
            block = block + factor[:, j : j + 1] * term
        blocks.append(block.astype(bf16))
    attended = jnp.concatenate(blocks, axis=1)
    part = jnp.dot(attended, w_out[...], preferred_element_type=f32)
    first = (lax.axis_index("head") == 0).astype(f32)
    part = (part + tok[...].astype(f32) * first).astype(bf16)
    for g in range(out.shape[0]):
        out[g] = part


def mix_kernel(head_size, pieces, gain, w_in, taps, bias, state, w_xproj, *outs):
    proj, u_out, gate_out, mid_out = outs
    group, rows, cols = pieces.shape
    blocks = []
    squares = 0.0
    for s in range(group // head_size):
        block = pieces[s * head_size].astype(f32)
        for h in range(1, head_size):
            block = block + pieces[s * head_size + h].astype(f32)
        blocks.append(block)
        squares = squares + jnp.sum(block * block, axis=1, keepdims=True)
    here = lax.axis_index("seq")
    own = blocks[0]
    for s in range(1, len(blocks)):
        own = jnp.where(here == s, blocks[s], own)
    mid_out[...] = own
    inv_rms = lax.rsqrt(squares / (cols * len(blocks)) + norm_eps)
    inner = 0.0
    gate = 0.0
    for s, block in enumerate(blocks):
        span = slice(s * cols, (s + 1) * cols)
        lifted = (block * inv_rms * gain[:, span]).astype(bf16)
        inner = inner + jnp.dot(lifted, w_in[0, span], preferred_element_type=f32)
        gate = gate + jnp.dot(lifted, w_in[1, span], preferred_element_type=f32)
    last = state.shape[0]
    mixed = inner * taps[last : last + 1, :] + bias[...]
    for k in range(last):
        mixed = mixed + state[k] * taps[k : k + 1, :]
    active = mixed / (1.0 + jnp.exp(-mixed))
    u_out[...] = active
    gate_out[...] = gate / (1.0 + jnp.exp(-gate))
    part = lax.dot_general(
        active.astype(bf16), w_xproj[...], (((1,), (1,)), ((), ())), preferred_element_type=f32
    )
    for g in range(proj.shape[0]):
        proj[g] = part


def state_kernel(
    head_size, pieces, w_dt, dt_bias, a_log, skip, state, u, gate, w_out, new_state, out
):
    rows, states, channels = state.shape
    rank = w_dt.shape[0]
    total = pieces[0]
    for g in range(1, pieces.shape[0]):
        total = total + pieces[g]
    maps = total[:, rank : rank + 2 * states]
    maps = jnp.concatenate([maps, jnp.zeros((rows, LANES - 2 * states), f32)], axis=1)
    maps = jnp.concatenate([maps, jnp.zeros((LANES - rows, LANES), f32)], axis=0).T
    raw = (
        jnp.dot(total[:, :rank].astype(bf16), w_dt[...], preferred_element_type=f32) + dt_bias[...]
    )
    step = jnp.maximum(raw, 0.0) + jnp.log1p(jnp.exp(-jnp.abs(raw)))
    rate = -jnp.exp(a_log[...])
    active = u[...]
    scaled = step * active
    lines = []
    for b in range(rows):
        fresh = jnp.exp(step[b : b + 1] * rate) * state[b] + scaled[b : b + 1] * maps[:states, b : b + 1]
        new_state[b] = fresh
        lines.append(jnp.sum(fresh * maps[states : 2 * states, b : b + 1], axis=0, keepdims=True))
    readout = jnp.concatenate(lines, axis=0) + skip[...] * active
    gated = (readout * gate[...]).astype(bf16)
    cols = out.shape[2]
    for s in range(out.shape[0] // head_size):
        part = jnp.dot(
            gated, w_out[:, s * cols : (s + 1) * cols], preferred_element_type=f32
        ).astype(bf16)
        for h in range(head_size):
            out[s * head_size + h] = part


def finish_kernel(mid, pieces, out):
    total = pieces[0].astype(f32)
    for g in range(1, pieces.shape[0]):
        total = total + pieces[g].astype(f32)
    out[...] = (mid[...] + total).astype(bf16)


def local(
    tokens,
    attn_gain,
    w_query,
    key_projection_weight,
    value_projection_weight,
    w_attn_out,
    cache_keys,
    stored_value_cache,
    lengths,
    positions,
    mamba_gain,
    w_in,
    conv_weight,
    conv_bias,
    conv_state,
    w_xproj,
    w_dt,
    dt_bias,
    a_log,
    skip_gain,
    ssm_state,
    w_mamba_out,
):
    shape = jax.ShapeDtypeStruct
    mib = 2**20
    rows, cols = tokens.shape
    head_dim = cache_keys.shape[3]
    kv_heads = cache_keys.shape[1]
    depth = cache_keys.shape[2]
    q_width = w_query.shape[1]
    kv_width = kv_heads * head_dim
    total_width = q_width + 2 * kv_width
    heads = q_width // head_dim
    seq_size = lax.axis_size("seq")
    head_size = lax.axis_size("head")
    group = seq_size * head_size
    width = cols * seq_size
    channels = w_dt.shape[1]
    mapped = w_xproj.shape[1]

    chunks = 4
    sent, part, square, cosine, sine = call(
        functools.partial(project_kernel, chunks),
        (
            shape((rows, total_width + LANES), bf16),
            shape((rows, total_width), f32),
            shape((rows, LANES), f32),
            shape((rows, head_dim), f32),
            shape((rows, head_dim), f32),
        ),
        (
            tokens,
            attn_gain[None],
            positions,
            far(w_query),
            far(key_projection_weight),
            far(value_projection_weight),
        ),
        "project",
        10 * mib,
        2 * rows * cols * total_width,
        scratch=[
            pltpu.VMEM(w_query.shape, bf16),
            pltpu.VMEM(key_projection_weight.shape, bf16),
            pltpu.VMEM(value_projection_weight.shape, bf16),
            pltpu.SemaphoreType.DMA((3, chunks)),
        ],
        spaces=[in_vmem, in_vmem, in_smem, in_any, in_any, in_any],
    )
    others = from_partners(sent, "seq")
    sent, mean, level, score_new, value_new = call(
        functools.partial(attend_kernel, width, seq_size),
        (
            shape((rows, q_width + LANES), bf16),
            shape((rows, q_width), f32),
            shape((rows, LANES), f32),
            shape((rows, LANES), f32),
            shape((rows, kv_width), f32),
        ),
        (part, square, *others, cosine, sine, lengths, cache_keys, stored_value_cache),
        "attend",
        LIMITS[0] * mib,
        4 * rows * q_width * depth,
        spaces=[in_vmem] * (3 + seq_size) + [in_smem, in_vmem, in_vmem],
    )
    others = from_partners(sent, "seq")
    (out,) = call(
        functools.partial(merge_kernel, heads, seq_size),
        (shape((group, rows, cols), bf16),),
        (mean, level, *others, score_new, value_new, tokens, w_attn_out),
        "merge",
        LIMITS[1] * mib,
        2 * rows * q_width * cols,
    )
    pieces = from_group(out)
    proj, active, gate, mid = call(
        functools.partial(mix_kernel, head_size),
        (
            shape((group, rows, mapped), f32),
            shape((rows, channels), f32),
            shape((rows, channels), f32),
            shape((rows, cols), f32),
        ),
        (
            pieces,
            mamba_gain[None],
            w_in,
            conv_weight,
            conv_bias[None],
            conv_state.transpose(1, 0, 2),
            w_xproj.T,
        ),
        "mix",
        LIMITS[2] * mib,
        4 * rows * width * channels,
    )
    new_state, out = call(
        functools.partial(state_kernel, head_size),
        (shape(ssm_state.shape, f32), shape((group, rows, cols), bf16)),
        (
            from_group(proj),
            w_dt,
            dt_bias[None],
            a_log,
            skip_gain[None],
            ssm_state,
            active,
            gate,
            w_mamba_out,
        ),
        "state",
        LIMITS[3] * mib,
        2 * rows * width * channels,
    )
    (hidden_out,) = call(
        finish_kernel,
        (shape((rows, cols), bf16),),
        (mid, from_group(out)),
        "finish",
        2 * mib,
        rows * cols * group,
    )
    return (hidden_out, new_state)


LIMITS = (4, 4, 4, 4)


def solution(mesh):
    in_specs = (
        P(("rep", "sub"), "seq"),
        P("seq"),
        P("seq", "head"),
        P("seq", "head"),
        P("seq", "head"),
        P("head", "seq"),
        P(("rep", "sub"), "head", "seq", None),
        P(("rep", "sub"), "head", "seq", None),
        P(("rep", "sub")),
        P(("rep", "sub")),
        P(),
        P(None, None, ("seq", "head")),
        P(None, ("seq", "head")),
        P(("seq", "head")),
        P(("rep", "sub"), None, ("seq", "head")),
        P(("seq", "head"), None),
        P(None, ("seq", "head")),
        P(("seq", "head")),
        P(None, ("seq", "head")),
        P(("seq", "head")),
        P(("rep", "sub"), None, ("seq", "head")),
        P(("seq", "head"), None),
    )
    out_specs = (P(("rep", "sub"), "seq"), P(("rep", "sub"), None, ("seq", "head")))
    return jax.shard_map(local, mesh=mesh, in_specs=in_specs, out_specs=out_specs, check_vma=False)
```

```python
import functools
import math

import jax
import jax.numpy as jnp
from jax import lax
from jax.experimental import pallas as pl
from jax.experimental.pallas import tpu as pltpu
from jax.sharding import PartitionSpec as P


norm_eps = 1e-05
masked_floor = -1e30
rope_base = 10000.0
group_axes = ("seq", "head")


def paired(count):
    return count & (count - 1) == 0 and count <= 4


def partner(index, step, count):
    if paired(count):
        return lax.bitwise_xor(index, step)
    return lax.rem(index + step, count)


def from_partners(values, axis):
    count = lax.axis_size(axis)
    result = []
    for k in range(1, count):
        pairs = [(i, i ^ k if paired(count) else (i + k) % count) for i in range(count)]
        result.append(held(lax.ppermute(values[k - 1], axis, pairs)))
    return result


def from_group(value):
    return lax.all_to_all(value, group_axes, 0, 0, tiled=False)


f32 = jnp.float32
bf16 = jnp.bfloat16
LANES = 128
WEIGHT = 10**12
in_vmem = pl.BlockSpec(memory_space=pltpu.VMEM)
in_smem = pl.BlockSpec(memory_space=pltpu.SMEM)
in_any = pl.BlockSpec(memory_space=pl.ANY)


def held(value):
    return pltpu.with_memory_space_constraint(value, pltpu.VMEM)


def far(value):
    return pltpu.with_memory_space_constraint(value, pltpu.HBM)


def call(kernel, out_shape, operands, limit, scratch=(), spaces=None, aliases={}):
    size = sum(math.prod(x.shape) * x.dtype.itemsize for x in operands)
    return pl.pallas_call(
        kernel,
        out_shape=out_shape,
        in_specs=spaces or [in_vmem] * len(operands),
        out_specs=jax.tree.map(lambda _: in_vmem, out_shape),
        scratch_shapes=scratch,
        input_output_aliases=aliases,
        cost_estimate=pl.CostEstimate(flops=WEIGHT, bytes_accessed=size, transcendentals=0),
        compiler_params=pltpu.CompilerParams(vmem_limit_bytes=limit),
    )(*operands)


def column(ref, rows):
    row = lax.broadcasted_iota(jnp.int32, (rows, LANES), 0)
    result = jnp.zeros((rows, LANES), jnp.int32)
    for b in range(rows):
        result = jnp.where(row == b, ref[b], result)
    return result


def in_three(value):
    high = value.astype(bf16).astype(f32)
    rest = value - high
    middle = rest.astype(bf16).astype(f32)
    return high, middle, rest - middle


def project_kernel(chunks, share, count, tok, gain, positions, wq, wk, wv, *refs):
    outs, scratch = refs[:-7], refs[-7:]
    sents = outs[: count - 1]
    part, fresh, square, cosine, sine = outs[count - 1 :]
    tok_buf, gain_buf, positions_buf, wq_buf, wk_buf, wv_buf, sems = scratch
    rows, cols = tok.shape
    depth = cols // chunks
    head_dim = cosine.shape[1]
    small = []
    pairs = ((tok, tok_buf), (gain, gain_buf), (positions, positions_buf))
    for i, (source, target) in enumerate(pairs):
        small.append(pltpu.make_async_copy(source, target, sems.at[3, i]))
        small[-1].start()
    copies = []
    for c in range(chunks):
        span = pl.ds(c * depth, depth)
        for i, (source, target) in enumerate(((wq, wq_buf), (wk, wk_buf), (wv, wv_buf))):
            copy = pltpu.make_async_copy(source.at[span], target.at[span], sems.at[i, c])
            copy.start()
            copies.append(copy)
    for copy in small:
        copy.wait()
    value = tok_buf[...].astype(f32)
    lifted = (value * gain_buf[...]).astype(bf16)
    squares = jnp.sum(value * value, axis=1, keepdims=True)
    lane = lax.broadcasted_iota(jnp.int32, (rows, LANES), 1)
    high, middle, low = in_three(squares)
    terms = jnp.where(lane == 0, high, jnp.where(lane == 1, middle, jnp.where(lane == 2, low, 0.0)))
    square[...] = jnp.broadcast_to(squares, (rows, LANES))
    half = head_dim // 2
    lane = lax.broadcasted_iota(jnp.int32, (rows, head_dim), 1)
    frequency = jnp.exp(-math.log(rope_base) / half * lax.rem(lane, half).astype(f32))
    angles = column(positions_buf, rows).astype(f32) * frequency
    cosine[...] = jnp.cos(angles)
    sine[...] = jnp.where(lane < half, -1.0, 1.0) * jnp.sin(angles)
    sums = [0.0, 0.0, 0.0]
    for c in range(chunks):
        x = lifted[:, c * depth : (c + 1) * depth]
        for i, buf in enumerate((wq_buf, wk_buf, wv_buf)):
            copies[3 * c + i].wait()
            sums[i] = sums[i] + jnp.dot(
                x, buf[c * depth : (c + 1) * depth], preferred_element_type=f32
            )
    query, key, value = sums
    q_width = query.shape[1]
    part[...] = query
    rounded = query.astype(bf16)
    here = lax.axis_index("seq")

    def pick(total, owner, c):
        result = total[:, :head_dim]
        for h in range(1, total.shape[1] // head_dim):
            block = total[:, h * head_dim : (h + 1) * head_dim]
            result = jnp.where(owner * share + c == h, block, result)
        return result

    for k in range(count):
        owner = here if k == 0 else partner(here, k, count)
        blocks = [pick(total, owner, c) for total in (key, value) for c in range(share)]
        blocks = jnp.concatenate(blocks, axis=1)
        if k == 0:
            fresh[...] = blocks
        else:
            sent = sents[k - 1]
            sent[:, :q_width] = rounded
            sent[:, q_width : q_width + blocks.shape[1]] = blocks.astype(bf16)
            sent[:, q_width + blocks.shape[1] :] = terms.astype(bf16)


def gate_kernel(*refs):
    pass


def attend_kernel(width, share, count, *refs):
    part, fresh, square = refs[:3]
    others = refs[3 : 2 + count]
    cosine, sine, lengths, keys, values = refs[2 + count : 7 + count]
    sent, mean_out, level_out = refs[7 + count :]
    rows, q_width = part.shape
    kv_heads, depth, head_dim = keys.shape[1:]
    heads = q_width // head_dim
    per_kv = heads // kv_heads
    scale = head_dim ** (-0.5)
    here = lax.axis_index("seq")
    squares = square[...]
    for other in others:
        terms = other[:, other.shape[1] - LANES :].astype(f32)
        squares = squares + jnp.sum(terms, axis=1, keepdims=True)
    inv_rms = lax.rsqrt(squares / width + norm_eps)

    def summed(own, own_start, start):
        total = own[:, own_start : own_start + head_dim]
        for other in others:
            total = total + other[:, start : start + head_dim].astype(f32)
        return total * inv_rms

    def rotated(x):
        x = x * cosine[...] + pltpu.roll(x, head_dim // 2, 1) * sine[...]
        return x.astype(bf16).astype(f32)

    tall = per_kv * rows
    owner = lax.rem(lax.broadcasted_iota(jnp.int32, (tall, depth), 0), rows)
    narrow = lax.rem(lax.broadcasted_iota(jnp.int32, (tall, head_dim), 0), rows)
    slot = lax.broadcasted_iota(jnp.int32, (tall, depth), 1)
    limit = column(lengths, rows)[:, :1] - here * depth
    live = slot < jnp.concatenate([limit] * per_kv, axis=0)
    lane = lax.broadcasted_iota(jnp.int32, (rows, LANES), 1)
    new_keys = []
    new_values = []
    for c in range(share):
        start = c * head_dim
        x = rotated(summed(fresh, start, q_width + start))
        new_keys.append(jnp.concatenate([x] * per_kv, axis=0))
        start = (share + c) * head_dim
        x = summed(fresh, start, q_width + start).astype(bf16).astype(f32)
        new_values.append(jnp.concatenate([x] * per_kv, axis=0))
    levels = jnp.zeros((rows, LANES), f32)
    together = 2 if kv_heads % 2 == 0 else 1
    for base in range(0, kv_heads, together):
        weights, tops, news, totals = [], [], [], []
        for h in range(base, base + together):
            stacked = [
                rotated(summed(part, start, start))
                for start in range(h * per_kv * head_dim, (h + 1) * per_kv * head_dim, head_dim)
            ]
            stacked = jnp.concatenate(stacked, axis=0)
            mine = (here == h // share).astype(f32)
            score_new = jnp.sum(stacked * new_keys[h % share], axis=1, keepdims=True) * scale
            score_new = score_new * mine + masked_floor * (1.0 - mine)
            scores = jnp.zeros((tall, depth), f32)
            for b in range(0, rows, 2):
                both = range(b, min(b + 2, rows))
                left = [jnp.where(narrow == i, stacked, 0.0) for i in both]
                scores = scores + lax.dot_general(
                    jnp.concatenate(left, axis=1).astype(bf16),
                    jnp.concatenate([keys[i, h] for i in both], axis=1),
                    (((1,), (1,)), ((), ())),
                    preferred_element_type=f32,
                )
            scores = jnp.where(live, scores * scale, masked_floor)
            top = jnp.maximum(jnp.max(scores, axis=1, keepdims=True), score_new)
            weight = jnp.where(live, jnp.exp(scores - top), 0.0)
            new = jnp.exp(score_new - top) * mine
            weights.append(weight)
            tops.append(top)
            news.append(new)
            totals.append(jnp.sum(weight, axis=1, keepdims=True) + new)
        acc = jnp.zeros((together * tall, together * head_dim), f32)
        for b in range(rows):
            left = [jnp.where(owner == b, weight, 0.0).astype(bf16) for weight in weights]
            acc = acc + jnp.dot(
                jnp.concatenate(left, axis=0),
                jnp.concatenate([values[b, base + i] for i in range(together)], axis=1),
                preferred_element_type=f32,
            )
        for i in range(together):
            mean = acc[i * tall : (i + 1) * tall, i * head_dim : (i + 1) * head_dim]
            mean = mean + news[i] * new_values[(base + i) % share]
            some = totals[i] > 0.0
            safe = jnp.where(some, totals[i], 1.0)
            level = jnp.where(some, tops[i] + jnp.log(safe), masked_floor)
            mean = mean / safe
            for j in range(per_kv):
                head = (base + i) * per_kv + j
                block = mean[j * rows : (j + 1) * rows]
                mean_out[:, head * head_dim : (head + 1) * head_dim] = block
                sent[:, head * head_dim : (head + 1) * head_dim] = block.astype(bf16)
                levels = jnp.where(lane == head, level[j * rows : (j + 1) * rows], levels)
    level_out[...] = levels
    high, middle, low = in_three(levels)
    packed = high + pltpu.roll(middle, heads, 1) + pltpu.roll(low, 2 * heads, 1)
    sent[:, q_width : q_width + LANES] = packed.astype(bf16)


def merge_kernel(heads, count, *refs):
    mean, level = refs[0], refs[1]
    others = refs[2 : 1 + count]
    tok, w_out, out = refs[1 + count :]
    _, q_width = mean.shape
    head_dim = q_width // heads
    levels = [level[...]]
    for other in others:
        packed = other[:, q_width : q_width + LANES].astype(f32)
        levels.append(
            (packed + pltpu.roll(packed, LANES - heads, 1))
            + pltpu.roll(packed, LANES - 2 * heads, 1)
        )
    top = functools.reduce(jnp.maximum, levels)
    factors = [jnp.exp(x - top) for x in levels]
    total = functools.reduce(jnp.add, factors)
    factors = [x / total for x in factors]
    blocks = []
    for j in range(heads):
        span = slice(j * head_dim, (j + 1) * head_dim)
        terms = [mean[:, span]] + [other[:, span].astype(f32) for other in others]
        block = 0.0
        for factor, term in zip(factors, terms):
            block = block + factor[:, j : j + 1] * term
        blocks.append(block.astype(bf16))
    attended = jnp.concatenate(blocks, axis=1)
    part = jnp.dot(attended, w_out[...], preferred_element_type=f32)
    first = (lax.axis_index("head") == 0).astype(f32)
    part = (part + tok[...].astype(f32) * first).astype(bf16)
    for g in range(out.shape[0]):
        out[g] = part


def mix_kernel(head_size, pieces, gain, w_in, taps, bias, state, w_xproj, *outs):
    proj, u_out, gate_out, mid_out = outs
    group, _, cols = pieces.shape
    blocks = []
    squares = 0.0
    for s in range(group // head_size):
        block = pieces[s * head_size].astype(f32)
        for h in range(1, head_size):
            block = block + pieces[s * head_size + h].astype(f32)
        blocks.append(block)
        squares = squares + jnp.sum(block * block, axis=1, keepdims=True)
    here = lax.axis_index("seq")
    own = blocks[0]
    for s in range(1, len(blocks)):
        own = jnp.where(here == s, blocks[s], own)
    mid_out[...] = own
    inv_rms = lax.rsqrt(squares / (cols * len(blocks)) + norm_eps)
    inner = 0.0
    gate = 0.0
    for s, block in enumerate(blocks):
        span = slice(s * cols, (s + 1) * cols)
        lifted = (block * inv_rms * gain[:, span]).astype(bf16)
        inner = inner + jnp.dot(lifted, w_in[0, span], preferred_element_type=f32)
        gate = gate + jnp.dot(lifted, w_in[1, span], preferred_element_type=f32)
    last = state.shape[0]
    mixed = inner * taps[last : last + 1, :] + bias[...]
    for k in range(last):
        mixed = mixed + state[k] * taps[k : k + 1, :]
    active = mixed / (1.0 + jnp.exp(-mixed))
    u_out[...] = active
    gate_out[...] = gate / (1.0 + jnp.exp(-gate))
    part = lax.dot_general(
        active.astype(bf16), w_xproj[...], (((1,), (1,)), ((), ())), preferred_element_type=f32
    )
    for g in range(proj.shape[0]):
        proj[g] = part


def state_kernel(
    head_size, pieces, w_dt, dt_bias, a_log, skip, state, u, gate, w_out, new_state, out
):
    rows, states, _ = state.shape
    rank = w_dt.shape[0]
    total = pieces[0]
    for g in range(1, pieces.shape[0]):
        total = total + pieces[g]
    maps = total[:, rank : rank + 2 * states]
    maps = jnp.concatenate([maps, jnp.zeros((rows, LANES - 2 * states), f32)], axis=1)
    maps = jnp.concatenate([maps, jnp.zeros((LANES - rows, LANES), f32)], axis=0).T
    raw = (
        jnp.dot(total[:, :rank].astype(bf16), w_dt[...], preferred_element_type=f32) + dt_bias[...]
    )
    step = jnp.maximum(raw, 0.0) + jnp.log1p(jnp.exp(-jnp.abs(raw)))
    rate = -jnp.exp(a_log[...])
    active = u[...]
    scaled = step * active
    lines = []
    for b in range(rows):
        fresh = jnp.exp(step[b : b + 1] * rate) * state[b] + scaled[b : b + 1] * maps[:states, b : b + 1]
        new_state[b] = fresh
        lines.append(jnp.sum(fresh * maps[states : 2 * states, b : b + 1], axis=0, keepdims=True))
    readout = jnp.concatenate(lines, axis=0) + skip[...] * active
    gated = (readout * gate[...]).astype(bf16)
    cols = out.shape[2]
    for s in range(out.shape[0] // head_size):
        part = jnp.dot(
            gated, w_out[:, s * cols : (s + 1) * cols], preferred_element_type=f32
        ).astype(bf16)
        for h in range(head_size):
            out[s * head_size + h] = part


def finish_kernel(mid, pieces, out):
    total = pieces[0].astype(f32)
    for g in range(1, pieces.shape[0]):
        total = total + pieces[g].astype(f32)
    out[...] = (mid[...] + total).astype(bf16)


def local(
    tokens,
    attn_gain,
    w_query,
    key_projection_weight,
    value_projection_weight,
    w_attn_out,
    cache_keys,
    stored_value_cache,
    lengths,
    positions,
    mamba_gain,
    w_in,
    conv_weight,
    conv_bias,
    conv_state,
    w_xproj,
    w_dt,
    dt_bias,
    a_log,
    skip_gain,
    ssm_state,
    w_mamba_out,
):
    shape = jax.ShapeDtypeStruct
    mib = 2**20
    rows, cols = tokens.shape
    head_dim = cache_keys.shape[3]
    kv_heads = cache_keys.shape[1]
    q_width = w_query.shape[1]
    heads = q_width // head_dim
    seq_size = lax.axis_size("seq")
    head_size = lax.axis_size("head")
    group = seq_size * head_size
    width = cols * seq_size
    channels = w_dt.shape[1]
    mapped = w_xproj.shape[1]

    chunks = 4
    share = -(-kv_heads // seq_size)
    owned = 2 * share * head_dim
    *sents, part, fresh, square, cosine, sine = call(
        functools.partial(project_kernel, chunks, share, seq_size),
        tuple(pltpu.VMEM((rows, q_width + owned + LANES), bf16) for _ in range(1, seq_size))
        + (
            shape((rows, q_width), f32),
            shape((rows, owned), f32),
            shape((rows, LANES), f32),
            shape((rows, head_dim), f32),
            shape((rows, head_dim), f32),
        ),
        (
            far(tokens),
            far(attn_gain[None]),
            far(positions),
            far(w_query),
            far(key_projection_weight),
            far(value_projection_weight),
        ),
        10 * mib,
        scratch=[
            pltpu.VMEM(tokens.shape, bf16),
            pltpu.VMEM((1, cols), f32),
            pltpu.SMEM(positions.shape, jnp.int32),
            pltpu.VMEM(w_query.shape, bf16),
            pltpu.VMEM(key_projection_weight.shape, bf16),
            pltpu.VMEM(value_projection_weight.shape, bf16),
            pltpu.SemaphoreType.DMA((4, chunks)),
        ],
        spaces=[in_any] * 6,
    )
    sents = call(
        gate_kernel,
        tuple(pltpu.VMEM(x.shape, x.dtype) for x in sents),
        tuple(held(x) for x in sents),
        mib,
        aliases={i: i for i in range(len(sents))},
    )
    others = from_partners(sents, "seq")
    sent, mean, level = call(
        functools.partial(attend_kernel, width, share, seq_size),
        (
            shape((rows, q_width + LANES), bf16),
            shape((rows, q_width), f32),
            shape((rows, LANES), f32),
        ),
        (part, fresh, square, *others, cosine, sine, lengths, cache_keys, stored_value_cache),
        LIMITS[0] * mib,
        spaces=[in_vmem] * (4 + seq_size) + [in_smem, in_vmem, in_vmem],
    )
    others = from_partners([sent] * (seq_size - 1), "seq")
    (out,) = call(
        functools.partial(merge_kernel, heads, seq_size),
        (shape((group, rows, cols), bf16),),
        (mean, level, *others, tokens, w_attn_out),
        LIMITS[1] * mib,
    )
    pieces = from_group(out)
    proj, active, gate, mid = call(
        functools.partial(mix_kernel, head_size),
        (
            shape((group, rows, mapped), f32),
            shape((rows, channels), f32),
            shape((rows, channels), f32),
            shape((rows, cols), f32),
        ),
        (
            pieces,
            mamba_gain[None],
            w_in,
            conv_weight,
            conv_bias[None],
            conv_state.transpose(1, 0, 2),
            w_xproj.T,
        ),
        LIMITS[2] * mib,
    )
    new_state, out = call(
        functools.partial(state_kernel, head_size),
        (shape(ssm_state.shape, f32), shape((group, rows, cols), bf16)),
        (
            from_group(proj),
            w_dt,
            dt_bias[None],
            a_log,
            skip_gain[None],
            ssm_state,
            active,
            gate,
            w_mamba_out,
        ),
        LIMITS[3] * mib,
    )
    (hidden_out,) = call(
        finish_kernel, (shape((rows, cols), bf16),), (mid, from_group(out)), 2 * mib
    )
    return (hidden_out, new_state)


LIMITS = (4, 4, 4, 4)


def solution(mesh):
    in_specs = (
        P(("rep", "sub"), "seq"),
        P("seq"),
        P("seq", "head"),
        P("seq", "head"),
        P("seq", "head"),
        P("head", "seq"),
        P(("rep", "sub"), "head", "seq", None),
        P(("rep", "sub"), "head", "seq", None),
        P(("rep", "sub")),
        P(("rep", "sub")),
        P(),
        P(None, None, ("seq", "head")),
        P(None, ("seq", "head")),
        P(("seq", "head")),
        P(("rep", "sub"), None, ("seq", "head")),
        P(("seq", "head"), None),
        P(None, ("seq", "head")),
        P(("seq", "head")),
        P(None, ("seq", "head")),
        P(("seq", "head")),
        P(("rep", "sub"), None, ("seq", "head")),
        P(("seq", "head"), None),
    )
    out_specs = (P(("rep", "sub"), "seq"), P(("rep", "sub"), None, ("seq", "head")))
    return jax.shard_map(local, mesh=mesh, in_specs=in_specs, out_specs=out_specs, check_vma=False)
```

```python
import functools
import math

import jax
import jax.numpy as jnp
from jax import lax
from jax.experimental import pallas as pl
from jax.experimental.pallas import tpu as pltpu
from jax.sharding import PartitionSpec as P


norm_eps = 1e-05
masked_floor = -1e30
rope_base = 10000.0
group_axes = ("seq", "head")


def paired(count):
    return count & (count - 1) == 0 and count <= 4


def partner(index, step, count):
    if paired(count):
        return lax.bitwise_xor(index, step)
    return lax.rem(index + step, count)


def from_partners(values, axis):
    count = lax.axis_size(axis)
    result = []
    for k in range(1, count):
        pairs = [(i, i ^ k if paired(count) else (i + k) % count) for i in range(count)]
        result.append(held(lax.ppermute(values[k - 1], axis, pairs)))
    return result


def from_group(value):
    return lax.all_to_all(value, group_axes, 0, 0, tiled=False)


f32 = jnp.float32
bf16 = jnp.bfloat16
LANES = 128
WEIGHT = 10**12
PIECE = 512
in_vmem = pl.BlockSpec(memory_space=pltpu.VMEM)
in_any = pl.BlockSpec(memory_space=pl.ANY)


def held(value):
    return pltpu.with_memory_space_constraint(value, pltpu.VMEM)


def far(value):
    return pltpu.with_memory_space_constraint(value, pltpu.HBM)


def call(kernel, out_shape, operands, limit, scratch=(), spaces=None, aliases={}):
    size = sum(math.prod(x.shape) * x.dtype.itemsize for x in operands)
    return pl.pallas_call(
        kernel,
        out_shape=out_shape,
        in_specs=spaces or [in_vmem] * len(operands),
        out_specs=jax.tree.map(lambda _: in_vmem, out_shape),
        scratch_shapes=scratch,
        input_output_aliases=aliases,
        cost_estimate=pl.CostEstimate(flops=WEIGHT, bytes_accessed=size, transcendentals=0),
        compiler_params=pltpu.CompilerParams(vmem_limit_bytes=limit),
    )(*operands)


def column(ref, rows):
    row = lax.broadcasted_iota(jnp.int32, (rows, LANES), 0)
    result = jnp.zeros((rows, LANES), jnp.int32)
    for b in range(rows):
        result = jnp.where(row == b, ref[b], result)
    return result


def in_three(value):
    high = value.astype(bf16).astype(f32)
    rest = value - high
    middle = rest.astype(bf16).astype(f32)
    return high, middle, rest - middle


def project_kernel(chunks, share, context, tok, gain, positions, lengths, wq, wk, wv, *refs):
    count = lax.axis_size("seq")
    outs, scratch = refs[:-8], refs[-8:]
    sents = outs[: count - 1]
    part, fresh, square, cosine, sine, limit = outs[count - 1 :]
    tok_buf, gain_buf, positions_buf, lengths_buf, wq_buf, wk_buf, wv_buf, sems = scratch
    rows, cols = tok.shape
    depth = cols // chunks
    head_dim = cosine.shape[1]
    small = []
    pairs = ((tok, tok_buf), (gain, gain_buf), (positions, positions_buf), (lengths, lengths_buf))
    for i, (source, target) in enumerate(pairs):
        small.append(pltpu.make_async_copy(source, target, sems.at[3, i]))
        small[-1].start()
    copies = []
    for c in range(chunks):
        span = pl.ds(c * depth, depth)
        for i, (source, target) in enumerate(((wq, wq_buf), (wk, wk_buf), (wv, wv_buf))):
            copy = pltpu.make_async_copy(source.at[span], target.at[span], sems.at[i, c])
            copy.start()
            copies.append(copy)
    for copy in small:
        copy.wait()
    value = tok_buf[...].astype(f32)
    lifted = (value * gain_buf[...]).astype(bf16)
    squares = jnp.sum(value * value, axis=1, keepdims=True)
    lane = lax.broadcasted_iota(jnp.int32, (rows, LANES), 1)
    high, middle, low = in_three(squares)
    terms = jnp.where(lane == 0, high, jnp.where(lane == 1, middle, jnp.where(lane == 2, low, 0.0)))
    square[...] = jnp.broadcast_to(squares, (rows, LANES))
    half = head_dim // 2
    lane = lax.broadcasted_iota(jnp.int32, (rows, head_dim), 1)
    frequency = jnp.exp(-math.log(rope_base) / half * lax.rem(lane, half).astype(f32))
    angles = column(positions_buf, rows).astype(f32) * frequency
    cosine[...] = jnp.cos(angles)
    sine[...] = jnp.where(lane < half, -1.0, 1.0) * jnp.sin(angles)
    here = lax.axis_index("seq")
    limit[...] = column(lengths_buf, rows) - here * context
    sums = [0.0, 0.0, 0.0]
    for c in range(chunks):
        x = lifted[:, c * depth : (c + 1) * depth]
        for i, buf in enumerate((wq_buf, wk_buf, wv_buf)):
            copies[3 * c + i].wait()
            sums[i] = sums[i] + jnp.dot(
                x, buf[c * depth : (c + 1) * depth], preferred_element_type=f32
            )
    query, key, value = sums
    q_width = query.shape[1]
    part[...] = query
    rounded = query.astype(bf16)

    def pick(total, owner, c):
        result = total[:, :head_dim]
        for h in range(1, total.shape[1] // head_dim):
            block = total[:, h * head_dim : (h + 1) * head_dim]
            result = jnp.where(owner * share + c == h, block, result)
        return result

    for k in range(count):
        owner = here if k == 0 else partner(here, k, count)
        blocks = [pick(total, owner, c) for total in (key, value) for c in range(share)]
        blocks = jnp.concatenate(blocks, axis=1)
        if k == 0:
            fresh[...] = blocks
        else:
            sent = sents[k - 1]
            sent[:, :q_width] = rounded
            sent[:, q_width : q_width + blocks.shape[1]] = blocks.astype(bf16)
            sent[:, q_width + blocks.shape[1] :] = terms.astype(bf16)


def gate_kernel(*refs):
    pass


def attend_kernel(width, share, count, *refs):
    part, fresh, square = refs[:3]
    others = refs[3 : 2 + count]
    cosine, sine, limit, keys, values = refs[2 + count : 7 + count]
    sent, mean_out, level_out = refs[7 + count :]
    rows, q_width = part.shape
    kv_heads, depth, head_dim = keys.shape[1:]
    heads = q_width // head_dim
    per_kv = heads // kv_heads
    scale = head_dim ** (-0.5)
    here = lax.axis_index("seq")
    squares = square[...]
    for other in others:
        terms = other[:, other.shape[1] - LANES :].astype(f32)
        squares = squares + jnp.sum(terms, axis=1, keepdims=True)
    inv_rms = lax.rsqrt(squares / width + norm_eps)

    def summed(own, own_start, start):
        total = own[:, own_start : own_start + head_dim]
        for other in others:
            total = total + other[:, start : start + head_dim].astype(f32)
        return total * inv_rms

    def rotated(x):
        x = x * cosine[...] + pltpu.roll(x, head_dim // 2, 1) * sine[...]
        return x.astype(bf16).astype(f32)

    tall = per_kv * rows
    owner = lax.rem(lax.broadcasted_iota(jnp.int32, (tall, depth), 0), rows)
    narrow = lax.rem(lax.broadcasted_iota(jnp.int32, (tall, head_dim), 0), rows)
    slot = lax.broadcasted_iota(jnp.int32, (tall, depth), 1)
    live = slot < jnp.concatenate([limit[:, :1]] * per_kv, axis=0)
    lane = lax.broadcasted_iota(jnp.int32, (rows, LANES), 1)
    new_keys = []
    new_values = []
    for c in range(share):
        start = c * head_dim
        x = rotated(summed(fresh, start, q_width + start))
        new_keys.append(jnp.concatenate([x] * per_kv, axis=0))
        start = (share + c) * head_dim
        x = summed(fresh, start, q_width + start).astype(bf16).astype(f32)
        new_values.append(jnp.concatenate([x] * per_kv, axis=0))
    levels = jnp.zeros((rows, LANES), f32)
    together = 2 if kv_heads % 2 == 0 else 1
    for base in range(0, kv_heads, together):
        weights, tops, news, totals = [], [], [], []
        for h in range(base, base + together):
            stacked = [
                rotated(summed(part, start, start))
                for start in range(h * per_kv * head_dim, (h + 1) * per_kv * head_dim, head_dim)
            ]
            stacked = jnp.concatenate(stacked, axis=0)
            mine = (here == h // share).astype(f32)
            score_new = jnp.sum(stacked * new_keys[h % share], axis=1, keepdims=True) * scale
            score_new = score_new * mine + masked_floor * (1.0 - mine)
            scores = jnp.zeros((tall, depth), f32)
            for b in range(0, rows, 2):
                both = range(b, min(b + 2, rows))
                left = [jnp.where(narrow == i, stacked, 0.0) for i in both]
                scores = scores + lax.dot_general(
                    jnp.concatenate(left, axis=1).astype(bf16),
                    jnp.concatenate([keys[i, h] for i in both], axis=1),
                    (((1,), (1,)), ((), ())),
                    preferred_element_type=f32,
                )
            scores = jnp.where(live, scores * scale, masked_floor)
            top = jnp.maximum(jnp.max(scores, axis=1, keepdims=True), score_new)
            weight = jnp.where(live, jnp.exp(scores - top), 0.0)
            new = jnp.exp(score_new - top) * mine
            weights.append(weight)
            tops.append(top)
            news.append(new)
            totals.append(jnp.sum(weight, axis=1, keepdims=True) + new)
        acc = jnp.zeros((together * tall, together * head_dim), f32)
        for b in range(rows):
            left = [jnp.where(owner == b, weight, 0.0).astype(bf16) for weight in weights]
            acc = acc + jnp.dot(
                jnp.concatenate(left, axis=0),
                jnp.concatenate([values[b, base + i] for i in range(together)], axis=1),
                preferred_element_type=f32,
            )
        for i in range(together):
            mean = acc[i * tall : (i + 1) * tall, i * head_dim : (i + 1) * head_dim]
            mean = mean + news[i] * new_values[(base + i) % share]
            some = totals[i] > 0.0
            safe = jnp.where(some, totals[i], 1.0)
            level = jnp.where(some, tops[i] + jnp.log(safe), masked_floor)
            mean = mean / safe
            for j in range(per_kv):
                head = (base + i) * per_kv + j
                block = mean[j * rows : (j + 1) * rows]
                mean_out[:, head * head_dim : (head + 1) * head_dim] = block
                sent[:, head * head_dim : (head + 1) * head_dim] = block.astype(bf16)
                levels = jnp.where(lane == head, level[j * rows : (j + 1) * rows], levels)
    level_out[...] = levels
    high, middle, low = in_three(levels)
    packed = high + pltpu.roll(middle, heads, 1) + pltpu.roll(low, 2 * heads, 1)
    sent[:, q_width : q_width + LANES] = packed.astype(bf16)


def merge_kernel(heads, count, *refs):
    mean, level = refs[0], refs[1]
    others = refs[2 : 1 + count]
    tok, w_out, out = refs[1 + count :]
    _, q_width = mean.shape
    head_dim = q_width // heads
    levels = [level[...]]
    for other in others:
        packed = other[:, q_width : q_width + LANES].astype(f32)
        levels.append(
            (packed + pltpu.roll(packed, LANES - heads, 1))
            + pltpu.roll(packed, LANES - 2 * heads, 1)
        )
    top = functools.reduce(jnp.maximum, levels)
    factors = [jnp.exp(x - top) for x in levels]
    total = functools.reduce(jnp.add, factors)
    factors = [x / total for x in factors]
    blocks = []
    for j in range(heads):
        span = slice(j * head_dim, (j + 1) * head_dim)
        terms = [mean[:, span]] + [other[:, span].astype(f32) for other in others]
        block = 0.0
        for factor, term in zip(factors, terms):
            block = block + factor[:, j : j + 1] * term
        blocks.append(block.astype(bf16))
    attended = jnp.concatenate(blocks, axis=1)
    part = jnp.dot(attended, w_out[...], preferred_element_type=f32)
    first = (lax.axis_index("head") == 0).astype(f32)
    part = (part + tok[...].astype(f32) * first).astype(bf16)
    for g in range(out.shape[0]):
        out[g] = part


def mix_kernel(head_size, pieces, gain, w_in, taps, bias, state, w_xproj, *outs):
    proj, u_out, gate_out, mid_out = outs
    group, _, cols = pieces.shape
    blocks = []
    squares = 0.0
    for s in range(group // head_size):
        block = pieces[s * head_size].astype(f32)
        for h in range(1, head_size):
            block = block + pieces[s * head_size + h].astype(f32)
        blocks.append(block)
        squares = squares + jnp.sum(block * block, axis=1, keepdims=True)
    here = lax.axis_index("seq")
    own = blocks[0]
    for s in range(1, len(blocks)):
        own = jnp.where(here == s, blocks[s], own)
    mid_out[...] = own
    inv_rms = lax.rsqrt(squares / (cols * len(blocks)) + norm_eps)
    inner = 0.0
    gate = 0.0
    for s, block in enumerate(blocks):
        span = slice(s * cols, (s + 1) * cols)
        lifted = (block * inv_rms * gain[:, span]).astype(bf16)
        inner = inner + jnp.dot(lifted, w_in[0, span], preferred_element_type=f32)
        gate = gate + jnp.dot(lifted, w_in[1, span], preferred_element_type=f32)
    last = state.shape[0]
    mixed = inner * taps[last : last + 1, :] + bias[...]
    for k in range(last):
        mixed = mixed + state[k] * taps[k : k + 1, :]
    active = mixed / (1.0 + jnp.exp(-mixed))
    u_out[...] = active
    gate_out[...] = gate / (1.0 + jnp.exp(-gate))
    part = lax.dot_general(
        active.astype(bf16), w_xproj[...], (((1,), (1,)), ((), ())), preferred_element_type=f32
    )
    for g in range(proj.shape[0]):
        proj[g] = part


def state_kernel(
    head_size, pieces, w_dt, dt_bias, a_log, skip, state, u, gate, w_out, new_state, out
):
    rows, states, channels = state.shape
    rank = w_dt.shape[0]
    total = pieces[0]
    for g in range(1, pieces.shape[0]):
        total = total + pieces[g]
    maps = total[:, rank : rank + 2 * states]
    maps = jnp.concatenate([maps, jnp.zeros((rows, LANES - 2 * states), f32)], axis=1)
    maps = jnp.concatenate([maps, jnp.zeros((LANES - rows, LANES), f32)], axis=0).T
    low = total[:, :rank].astype(bf16)
    cols = out.shape[2]
    parts = [0.0] * (out.shape[0] // head_size)
    piece = min(channels, PIECE)
    for start in range(0, channels, piece):
        span = slice(start, start + piece)
        raw = jnp.dot(low, w_dt[:, span], preferred_element_type=f32) + dt_bias[:, span]
        step = jnp.maximum(raw, 0.0) + jnp.log1p(jnp.exp(-jnp.abs(raw)))
        rate = -jnp.exp(a_log[:, span])
        active = u[:, span]
        scaled = step * active
        lines = []
        for b in range(rows):
            fresh = jnp.exp(step[b : b + 1] * rate) * state[b, :, span]
            fresh = fresh + scaled[b : b + 1] * maps[:states, b : b + 1]
            new_state[b, :, span] = fresh
            lines.append(
                jnp.sum(fresh * maps[states : 2 * states, b : b + 1], axis=0, keepdims=True)
            )
        readout = jnp.concatenate(lines, axis=0) + skip[:, span] * active
        gated = (readout * gate[:, span]).astype(bf16)
        for s in range(len(parts)):
            parts[s] = parts[s] + jnp.dot(
                gated, w_out[span, s * cols : (s + 1) * cols], preferred_element_type=f32
            )
    for s, part in enumerate(parts):
        part = part.astype(bf16)
        for h in range(head_size):
            out[s * head_size + h] = part


def finish_kernel(mid, pieces, out):
    total = pieces[0].astype(f32)
    for g in range(1, pieces.shape[0]):
        total = total + pieces[g].astype(f32)
    out[...] = (mid[...] + total).astype(bf16)


def local(
    tokens,
    attn_gain,
    w_query,
    key_projection_weight,
    value_projection_weight,
    w_attn_out,
    cache_keys,
    stored_value_cache,
    lengths,
    positions,
    mamba_gain,
    w_in,
    conv_weight,
    conv_bias,
    conv_state,
    w_xproj,
    w_dt,
    dt_bias,
    a_log,
    skip_gain,
    ssm_state,
    w_mamba_out,
):
    shape = jax.ShapeDtypeStruct
    mib = 2**20
    rows, cols = tokens.shape
    head_dim = cache_keys.shape[3]
    kv_heads = cache_keys.shape[1]
    depth = cache_keys.shape[2]
    q_width = w_query.shape[1]
    heads = q_width // head_dim
    seq_size = lax.axis_size("seq")
    head_size = lax.axis_size("head")
    group = seq_size * head_size
    width = cols * seq_size
    channels = w_dt.shape[1]
    mapped = w_xproj.shape[1]

    chunks = 4
    share = -(-kv_heads // seq_size)
    owned = 2 * share * head_dim
    *sents, part, fresh, square, cosine, sine, limit = call(
        functools.partial(project_kernel, chunks, share, depth),
        tuple(pltpu.VMEM((rows, q_width + owned + LANES), bf16) for _ in range(1, seq_size))
        + (
            shape((rows, q_width), f32),
            shape((rows, owned), f32),
            shape((rows, LANES), f32),
            shape((rows, head_dim), f32),
            shape((rows, head_dim), f32),
            shape((rows, LANES), jnp.int32),
        ),
        (
            far(tokens),
            far(attn_gain[None]),
            far(positions),
            far(lengths),
            far(w_query),
            far(key_projection_weight),
            far(value_projection_weight),
        ),
        10 * mib,
        scratch=[
            pltpu.VMEM(tokens.shape, bf16),
            pltpu.VMEM((1, cols), f32),
            pltpu.SMEM(positions.shape, jnp.int32),
            pltpu.SMEM(lengths.shape, jnp.int32),
            pltpu.VMEM(w_query.shape, bf16),
            pltpu.VMEM(key_projection_weight.shape, bf16),
            pltpu.VMEM(value_projection_weight.shape, bf16),
            pltpu.SemaphoreType.DMA((4, chunks)),
        ],
        spaces=[in_any] * 7,
    )
    sents = call(
        gate_kernel,
        tuple(pltpu.VMEM(x.shape, x.dtype) for x in sents),
        tuple(held(x) for x in sents),
        mib,
        aliases={i: i for i in range(len(sents))},
    )
    others = from_partners(sents, "seq")
    sent, mean, level = call(
        functools.partial(attend_kernel, width, share, seq_size),
        (
            shape((rows, q_width + LANES), bf16),
            shape((rows, q_width), f32),
            shape((rows, LANES), f32),
        ),
        (part, fresh, square, *others, cosine, sine, limit, cache_keys, stored_value_cache),
        LIMITS[0] * mib,
    )
    others = from_partners([sent] * (seq_size - 1), "seq")
    (out,) = call(
        functools.partial(merge_kernel, heads, seq_size),
        (shape((group, rows, cols), bf16),),
        (mean, level, *others, tokens, w_attn_out),
        LIMITS[1] * mib,
    )
    pieces = from_group(out)
    proj, active, gate, mid = call(
        functools.partial(mix_kernel, head_size),
        (
            shape((group, rows, mapped), f32),
            shape((rows, channels), f32),
            shape((rows, channels), f32),
            shape((rows, cols), f32),
        ),
        (
            pieces,
            mamba_gain[None],
            w_in,
            conv_weight,
            conv_bias[None],
            conv_state.transpose(1, 0, 2),
            w_xproj.T,
        ),
        LIMITS[2] * mib,
    )
    new_state, out = call(
        functools.partial(state_kernel, head_size),
        (shape(ssm_state.shape, f32), shape((group, rows, cols), bf16)),
        (
            from_group(proj),
            w_dt,
            dt_bias[None],
            a_log,
            skip_gain[None],
            ssm_state,
            active,
            gate,
            w_mamba_out,
        ),
        LIMITS[3] * mib,
    )
    (hidden_out,) = call(
        finish_kernel, (shape((rows, cols), bf16),), (mid, from_group(out)), 2 * mib
    )
    return (hidden_out, new_state)


LIMITS = (4, 4, 4, 4)


def solution(mesh):
    in_specs = (
        P(("rep", "sub"), "seq"),
        P("seq"),
        P("seq", "head"),
        P("seq", "head"),
        P("seq", "head"),
        P("head", "seq"),
        P(("rep", "sub"), "head", "seq", None),
        P(("rep", "sub"), "head", "seq", None),
        P(("rep", "sub")),
        P(("rep", "sub")),
        P(),
        P(None, None, ("seq", "head")),
        P(None, ("seq", "head")),
        P(("seq", "head")),
        P(("rep", "sub"), None, ("seq", "head")),
        P(("seq", "head"), None),
        P(None, ("seq", "head")),
        P(("seq", "head")),
        P(None, ("seq", "head")),
        P(("seq", "head")),
        P(("rep", "sub"), None, ("seq", "head")),
        P(("seq", "head"), None),
    )
    out_specs = (P(("rep", "sub"), "seq"), P(("rep", "sub"), None, ("seq", "head")))
    return jax.shard_map(local, mesh=mesh, in_specs=in_specs, out_specs=out_specs, check_vma=False)
```

```python
import functools
import math

import jax
import jax.numpy as jnp
from jax import lax
from jax.experimental import pallas as pl
from jax.experimental.pallas import tpu as pltpu
from jax.sharding import PartitionSpec as P


norm_eps = 1e-05
masked_floor = -1e30
rope_base = 10000.0
group_axes = ("seq", "head")


def paired(count):
    return count & (count - 1) == 0 and count <= 4


def partner(index, step, count):
    if paired(count):
        return lax.bitwise_xor(index, step)
    return lax.rem(index + step, count)


def from_partners(values, axis):
    count = lax.axis_size(axis)
    result = []
    for k in range(1, count):
        pairs = [(i, i ^ k if paired(count) else (i + k) % count) for i in range(count)]
        result.append(held(lax.ppermute(values[k - 1], axis, pairs)))
    return result


def from_group(value):
    return lax.all_to_all(value, group_axes, 0, 0, tiled=False)


f32 = jnp.float32
bf16 = jnp.bfloat16
LANES = 128
WEIGHT = 10**12
PIECE = 512
in_vmem = pl.BlockSpec(memory_space=pltpu.VMEM)
in_any = pl.BlockSpec(memory_space=pl.ANY)


def held(value):
    return pltpu.with_memory_space_constraint(value, pltpu.VMEM)


def far(value):
    return pltpu.with_memory_space_constraint(value, pltpu.HBM)


def call(kernel, out_shape, operands, limit, scratch=(), spaces=None, aliases={}):
    size = sum(math.prod(x.shape) * x.dtype.itemsize for x in operands)
    return pl.pallas_call(
        kernel,
        out_shape=out_shape,
        in_specs=spaces or [in_vmem] * len(operands),
        out_specs=jax.tree.map(lambda _: in_vmem, out_shape),
        scratch_shapes=scratch,
        input_output_aliases=aliases,
        cost_estimate=pl.CostEstimate(flops=WEIGHT, bytes_accessed=size, transcendentals=0),
        compiler_params=pltpu.CompilerParams(vmem_limit_bytes=limit),
    )(*operands)


def column(ref, rows):
    row = lax.broadcasted_iota(jnp.int32, (rows, LANES), 0)
    result = jnp.zeros((rows, LANES), jnp.int32)
    for b in range(rows):
        result = jnp.where(row == b, ref[b], result)
    return result


def in_three(value):
    high = value.astype(bf16).astype(f32)
    rest = value - high
    middle = rest.astype(bf16).astype(f32)
    return high, middle, rest - middle


def project_kernel(chunks, share, context, tok, gain, positions, lengths, wq, wk, wv, *refs):
    count = lax.axis_size("seq")
    outs, scratch = refs[:-8], refs[-8:]
    sents = outs[: count - 1]
    part, fresh, square, cosine, sine, limit = outs[count - 1 :]
    tok_buf, gain_buf, positions_buf, lengths_buf, wq_buf, wk_buf, wv_buf, sems = scratch
    rows, cols = tok.shape
    depth = cols // chunks
    head_dim = cosine.shape[1]
    small = []
    pairs = ((tok, tok_buf), (gain, gain_buf), (positions, positions_buf), (lengths, lengths_buf))
    for i, (source, target) in enumerate(pairs):
        small.append(pltpu.make_async_copy(source, target, sems.at[3, i]))
        small[-1].start()
    copies = []
    for i, (source, target) in enumerate(((wq, wq_buf), (wk, wk_buf), (wv, wv_buf))):
        for c in range(chunks):
            span = pl.ds(c * depth, depth)
            copy = pltpu.make_async_copy(source.at[span], target.at[span], sems.at[i, c])
            copy.start()
            copies.append(copy)
    for copy in small:
        copy.wait()
    value = tok_buf[...].astype(f32)
    lifted = (value * gain_buf[...]).astype(bf16)
    squares = jnp.sum(value * value, axis=1, keepdims=True)
    lane = lax.broadcasted_iota(jnp.int32, (rows, LANES), 1)
    high, middle, low = in_three(squares)
    terms = jnp.where(lane == 0, high, jnp.where(lane == 1, middle, jnp.where(lane == 2, low, 0.0)))
    square[...] = jnp.broadcast_to(squares, (rows, LANES))
    half = head_dim // 2
    lane = lax.broadcasted_iota(jnp.int32, (rows, head_dim), 1)
    frequency = jnp.exp(-math.log(rope_base) / half * lax.rem(lane, half).astype(f32))
    angles = column(positions_buf, rows).astype(f32) * frequency
    cosine[...] = jnp.cos(angles)
    sine[...] = jnp.where(lane < half, -1.0, 1.0) * jnp.sin(angles)
    here = lax.axis_index("seq")
    limit[...] = column(lengths_buf, rows) - here * context
    sums = [0.0, 0.0, 0.0]
    for i, buf in enumerate((wq_buf, wk_buf, wv_buf)):
        for c in range(chunks):
            x = lifted[:, c * depth : (c + 1) * depth]
            copies[chunks * i + c].wait()
            sums[i] = sums[i] + jnp.dot(
                x, buf[c * depth : (c + 1) * depth], preferred_element_type=f32
            )
    query, key, value = sums
    q_width = query.shape[1]
    part[...] = query
    rounded = query.astype(bf16)

    def pick(total, owner, c):
        result = total[:, :head_dim]
        for h in range(1, total.shape[1] // head_dim):
            block = total[:, h * head_dim : (h + 1) * head_dim]
            result = jnp.where(owner * share + c == h, block, result)
        return result

    for k in range(count):
        owner = here if k == 0 else partner(here, k, count)
        blocks = [pick(total, owner, c) for total in (key, value) for c in range(share)]
        blocks = jnp.concatenate(blocks, axis=1)
        if k == 0:
            fresh[...] = blocks
        else:
            sent = sents[k - 1]
            sent[:, :q_width] = rounded
            sent[:, q_width : q_width + blocks.shape[1]] = blocks.astype(bf16)
            sent[:, q_width + blocks.shape[1] :] = terms.astype(bf16)


def gate_kernel(*refs):
    pass


def attend_kernel(width, share, count, *refs):
    part, fresh, square = refs[:3]
    others = refs[3 : 2 + count]
    cosine, sine, limit, keys, values = refs[2 + count : 7 + count]
    sent, mean_out, level_out = refs[7 + count :]
    rows, q_width = part.shape
    kv_heads, depth, head_dim = keys.shape[1:]
    heads = q_width // head_dim
    per_kv = heads // kv_heads
    scale = head_dim ** (-0.5)
    here = lax.axis_index("seq")
    squares = square[...]
    for other in others:
        terms = other[:, other.shape[1] - LANES :].astype(f32)
        squares = squares + jnp.sum(terms, axis=1, keepdims=True)
    inv_rms = lax.rsqrt(squares / width + norm_eps)

    def summed(own, own_start, start):
        total = own[:, own_start : own_start + head_dim]
        for other in others:
            total = total + other[:, start : start + head_dim].astype(f32)
        return total * inv_rms

    def rotated(x):
        x = x * cosine[...] + pltpu.roll(x, head_dim // 2, 1) * sine[...]
        return x.astype(bf16).astype(f32)

    tall = per_kv * rows
    owner = lax.rem(lax.broadcasted_iota(jnp.int32, (tall, depth), 0), rows)
    narrow = lax.rem(lax.broadcasted_iota(jnp.int32, (tall, head_dim), 0), rows)
    slot = lax.broadcasted_iota(jnp.int32, (tall, depth), 1)
    live = slot < jnp.concatenate([limit[:, :1]] * per_kv, axis=0)
    lane = lax.broadcasted_iota(jnp.int32, (rows, LANES), 1)
    new_keys = []
    new_values = []
    for c in range(share):
        start = c * head_dim
        x = rotated(summed(fresh, start, q_width + start))
        new_keys.append(jnp.concatenate([x] * per_kv, axis=0))
        start = (share + c) * head_dim
        x = summed(fresh, start, q_width + start).astype(bf16).astype(f32)
        new_values.append(jnp.concatenate([x] * per_kv, axis=0))
    levels = jnp.zeros((rows, LANES), f32)
    together = 2 if kv_heads % 2 == 0 else 1
    raw, fresh_scores = [], []
    for h in range(kv_heads):
        stacked = [
            rotated(summed(part, start, start))
            for start in range(h * per_kv * head_dim, (h + 1) * per_kv * head_dim, head_dim)
        ]
        stacked = jnp.concatenate(stacked, axis=0)
        score_new = jnp.sum(stacked * new_keys[h % share], axis=1, keepdims=True) * scale
        scores = jnp.zeros((tall, depth), f32)
        for b in range(0, rows, 2):
            both = range(b, min(b + 2, rows))
            left = [jnp.where(narrow == i, stacked, 0.0) for i in both]
            scores = scores + lax.dot_general(
                jnp.concatenate(left, axis=1).astype(bf16),
                jnp.concatenate([keys[i, h] for i in both], axis=1),
                (((1,), (1,)), ((), ())),
                preferred_element_type=f32,
            )
        raw.append(scores)
        fresh_scores.append(score_new)
    for base in range(0, kv_heads, together):
        weights, tops, news, totals = [], [], [], []
        for h in range(base, base + together):
            mine = (here == h // share).astype(f32)
            score_new = fresh_scores[h] * mine + masked_floor * (1.0 - mine)
            scores = jnp.where(live, raw[h] * scale, masked_floor)
            top = jnp.maximum(jnp.max(scores, axis=1, keepdims=True), score_new)
            weight = jnp.where(live, jnp.exp(scores - top), 0.0)
            new = jnp.exp(score_new - top) * mine
            weights.append(weight)
            tops.append(top)
            news.append(new)
            totals.append(jnp.sum(weight, axis=1, keepdims=True) + new)
        acc = jnp.zeros((together * tall, together * head_dim), f32)
        for b in range(rows):
            left = [jnp.where(owner == b, weight, 0.0).astype(bf16) for weight in weights]
            acc = acc + jnp.dot(
                jnp.concatenate(left, axis=0),
                jnp.concatenate([values[b, base + i] for i in range(together)], axis=1),
                preferred_element_type=f32,
            )
        for i in range(together):
            mean = acc[i * tall : (i + 1) * tall, i * head_dim : (i + 1) * head_dim]
            mean = mean + news[i] * new_values[(base + i) % share]
            some = totals[i] > 0.0
            safe = jnp.where(some, totals[i], 1.0)
            level = jnp.where(some, tops[i] + jnp.log(safe), masked_floor)
            mean = mean / safe
            for j in range(per_kv):
                head = (base + i) * per_kv + j
                block = mean[j * rows : (j + 1) * rows]
                mean_out[:, head * head_dim : (head + 1) * head_dim] = block
                sent[:, head * head_dim : (head + 1) * head_dim] = block.astype(bf16)
                levels = jnp.where(lane == head, level[j * rows : (j + 1) * rows], levels)
    level_out[...] = levels
    high, middle, low = in_three(levels)
    packed = high + pltpu.roll(middle, heads, 1) + pltpu.roll(low, 2 * heads, 1)
    sent[:, q_width : q_width + LANES] = packed.astype(bf16)


def merge_kernel(heads, count, *refs):
    mean, level = refs[0], refs[1]
    others = refs[2 : 1 + count]
    tok, w_out, out = refs[1 + count :]
    _, q_width = mean.shape
    head_dim = q_width // heads
    levels = [level[...]]
    for other in others:
        packed = other[:, q_width : q_width + LANES].astype(f32)
        levels.append(
            (packed + pltpu.roll(packed, LANES - heads, 1))
            + pltpu.roll(packed, LANES - 2 * heads, 1)
        )
    top = functools.reduce(jnp.maximum, levels)
    factors = [jnp.exp(x - top) for x in levels]
    total = functools.reduce(jnp.add, factors)
    factors = [x / total for x in factors]
    blocks = []
    for j in range(heads):
        span = slice(j * head_dim, (j + 1) * head_dim)
        terms = [mean[:, span]] + [other[:, span].astype(f32) for other in others]
        block = 0.0
        for factor, term in zip(factors, terms):
            block = block + factor[:, j : j + 1] * term
        blocks.append(block.astype(bf16))
    attended = jnp.concatenate(blocks, axis=1)
    part = jnp.dot(attended, w_out[...], preferred_element_type=f32)
    first = (lax.axis_index("head") == 0).astype(f32)
    part = (part + tok[...].astype(f32) * first).astype(bf16)
    for g in range(out.shape[0]):
        out[g] = part


def mix_kernel(head_size, maps, pieces, gain, w_in, taps, bias, state, w_xproj, *outs):
    proj, u_out, gate_out, mid_out = outs
    group, rows, cols = pieces.shape
    blocks = []
    squares = 0.0
    for s in range(group // head_size):
        block = pieces[s * head_size].astype(f32)
        for h in range(1, head_size):
            block = block + pieces[s * head_size + h].astype(f32)
        blocks.append(block)
        squares = squares + jnp.sum(block * block, axis=1, keepdims=True)
    here = lax.axis_index("seq")
    own = blocks[0]
    for s in range(1, len(blocks)):
        own = jnp.where(here == s, blocks[s], own)
    mid_out[...] = own
    inv_rms = lax.rsqrt(squares / (cols * len(blocks)) + norm_eps)
    inner = 0.0
    gate = 0.0
    for s, block in enumerate(blocks):
        span = slice(s * cols, (s + 1) * cols)
        lifted = (block * inv_rms * gain[:, span]).astype(bf16)
        inner = inner + jnp.dot(lifted, w_in[0, span], preferred_element_type=f32)
        gate = gate + jnp.dot(lifted, w_in[1, span], preferred_element_type=f32)
    last = state.shape[0]
    mixed = inner * taps[last : last + 1, :] + bias[...]
    for k in range(last):
        mixed = mixed + state[k] * taps[k : k + 1, :]
    active = mixed / (1.0 + jnp.exp(-mixed))
    u_out[...] = active
    gate_out[...] = gate / (1.0 + jnp.exp(-gate))
    part = lax.dot_general(
        active.astype(bf16), w_xproj[...], (((1,), (1,)), ((), ())), preferred_element_type=f32
    )
    rows = part.shape[0]
    rank = part.shape[1] - maps
    tail = jnp.concatenate([part[:, rank:], jnp.zeros((rows, LANES - maps), f32)], axis=1)
    high, middle, low = in_three(tail)
    tail = high + pltpu.roll(middle, maps, 1) + pltpu.roll(low, 2 * maps, 1)
    part = jnp.concatenate([part[:, :rank], tail], axis=1).astype(bf16)
    for g in range(proj.shape[0]):
        proj[g] = part


def state_kernel(
    head_size, pieces, w_dt, dt_bias, a_log, skip, state, u, gate, w_out, new_state, out
):
    rows, states, channels = state.shape
    rank = w_dt.shape[0]
    total = pieces[0].astype(f32)
    for g in range(1, pieces.shape[0]):
        total = total + pieces[g].astype(f32)
    maps = total[:, rank:]
    maps = (
        maps
        + pltpu.roll(maps, LANES - 2 * states, 1)
        + pltpu.roll(maps, LANES - 4 * states, 1)
    )
    maps = jnp.concatenate([maps, jnp.zeros((LANES - rows, LANES), f32)], axis=0).T
    low = total[:, :rank].astype(bf16)
    cols = out.shape[2]
    parts = [0.0] * (out.shape[0] // head_size)
    piece = min(channels, PIECE)
    for start in range(0, channels, piece):
        span = slice(start, start + piece)
        raw = jnp.dot(low, w_dt[:, span], preferred_element_type=f32) + dt_bias[:, span]
        step = jnp.maximum(raw, 0.0) + jnp.log1p(jnp.exp(-jnp.abs(raw)))
        rate = -jnp.exp(a_log[:, span])
        active = u[:, span]
        scaled = step * active
        lines = []
        for b in range(rows):
            fresh = jnp.exp(step[b : b + 1] * rate) * state[b, :, span]
            fresh = fresh + scaled[b : b + 1] * maps[:states, b : b + 1]
            new_state[b, :, span] = fresh
            lines.append(
                jnp.sum(fresh * maps[states : 2 * states, b : b + 1], axis=0, keepdims=True)
            )
        readout = jnp.concatenate(lines, axis=0) + skip[:, span] * active
        gated = (readout * gate[:, span]).astype(bf16)
        for s in range(len(parts)):
            parts[s] = parts[s] + jnp.dot(
                gated, w_out[span, s * cols : (s + 1) * cols], preferred_element_type=f32
            )
    for s, part in enumerate(parts):
        part = part.astype(bf16)
        for h in range(head_size):
            out[s * head_size + h] = part


def finish_kernel(mid, pieces, out):
    total = pieces[0].astype(f32)
    for g in range(1, pieces.shape[0]):
        total = total + pieces[g].astype(f32)
    out[...] = (mid[...] + total).astype(bf16)


def local(
    tokens,
    attn_gain,
    w_query,
    key_projection_weight,
    value_projection_weight,
    w_attn_out,
    cache_keys,
    stored_value_cache,
    lengths,
    positions,
    mamba_gain,
    w_in,
    conv_weight,
    conv_bias,
    conv_state,
    w_xproj,
    w_dt,
    dt_bias,
    a_log,
    skip_gain,
    ssm_state,
    w_mamba_out,
):
    shape = jax.ShapeDtypeStruct
    mib = 2**20
    rows, cols = tokens.shape
    head_dim = cache_keys.shape[3]
    kv_heads = cache_keys.shape[1]
    depth = cache_keys.shape[2]
    q_width = w_query.shape[1]
    heads = q_width // head_dim
    seq_size = lax.axis_size("seq")
    head_size = lax.axis_size("head")
    group = seq_size * head_size
    width = cols * seq_size
    channels = w_dt.shape[1]
    mapped = w_xproj.shape[1]
    states = ssm_state.shape[1]

    chunks = 4
    share = -(-kv_heads // seq_size)
    owned = 2 * share * head_dim
    *sents, part, fresh, square, cosine, sine, limit = call(
        functools.partial(project_kernel, chunks, share, depth),
        tuple(pltpu.VMEM((rows, q_width + owned + LANES), bf16) for _ in range(1, seq_size))
        + (
            shape((rows, q_width), f32),
            shape((rows, owned), f32),
            shape((rows, LANES), f32),
            shape((rows, head_dim), f32),
            shape((rows, head_dim), f32),
            shape((rows, LANES), jnp.int32),
        ),
        (
            far(tokens),
            far(attn_gain[None]),
            far(positions),
            far(lengths),
            far(w_query),
            far(key_projection_weight),
            far(value_projection_weight),
        ),
        10 * mib,
        scratch=[
            pltpu.VMEM(tokens.shape, bf16),
            pltpu.VMEM((1, cols), f32),
            pltpu.SMEM(positions.shape, jnp.int32),
            pltpu.SMEM(lengths.shape, jnp.int32),
            pltpu.VMEM(w_query.shape, bf16),
            pltpu.VMEM(key_projection_weight.shape, bf16),
            pltpu.VMEM(value_projection_weight.shape, bf16),
            pltpu.SemaphoreType.DMA((4, chunks)),
        ],
        spaces=[in_any] * 7,
    )
    sents = call(
        gate_kernel,
        tuple(pltpu.VMEM(x.shape, x.dtype) for x in sents),
        tuple(held(x) for x in sents),
        mib,
        aliases={i: i for i in range(len(sents))},
    )
    others = from_partners(sents, "seq")
    sent, mean, level = call(
        functools.partial(attend_kernel, width, share, seq_size),
        (
            shape((rows, q_width + LANES), bf16),
            shape((rows, q_width), f32),
            shape((rows, LANES), f32),
        ),
        (part, fresh, square, *others, cosine, sine, limit, cache_keys, stored_value_cache),
        LIMITS[0] * mib,
    )
    others = from_partners([sent] * (seq_size - 1), "seq")
    (out,) = call(
        functools.partial(merge_kernel, heads, seq_size),
        (shape((group, rows, cols), bf16),),
        (mean, level, *others, tokens, w_attn_out),
        LIMITS[1] * mib,
    )
    pieces = from_group(out)
    proj, active, gate, mid = call(
        functools.partial(mix_kernel, head_size, 2 * states),
        (
            shape((group, rows, mapped - 2 * states + LANES), bf16),
            shape((rows, channels), f32),
            shape((rows, channels), f32),
            shape((rows, cols), f32),
        ),
        (
            pieces,
            mamba_gain[None],
            w_in,
            conv_weight,
            conv_bias[None],
            conv_state.transpose(1, 0, 2),
            w_xproj.T,
        ),
        LIMITS[2] * mib,
    )
    new_state, out = call(
        functools.partial(state_kernel, head_size),
        (shape(ssm_state.shape, f32), shape((group, rows, cols), bf16)),
        (
            from_group(proj),
            w_dt,
            dt_bias[None],
            a_log,
            skip_gain[None],
            ssm_state,
            active,
            gate,
            w_mamba_out,
        ),
        LIMITS[3] * mib,
    )
    (hidden_out,) = call(
        finish_kernel, (shape((rows, cols), bf16),), (mid, from_group(out)), 2 * mib
    )
    return (hidden_out, new_state)


LIMITS = (4, 4, 4, 4)


def solution(mesh):
    in_specs = (
        P(("rep", "sub"), "seq"),
        P("seq"),
        P("seq", "head"),
        P("seq", "head"),
        P("seq", "head"),
        P("head", "seq"),
        P(("rep", "sub"), "head", "seq", None),
        P(("rep", "sub"), "head", "seq", None),
        P(("rep", "sub")),
        P(("rep", "sub")),
        P(),
        P(None, None, ("seq", "head")),
        P(None, ("seq", "head")),
        P(("seq", "head")),
        P(("rep", "sub"), None, ("seq", "head")),
        P(("seq", "head"), None),
        P(None, ("seq", "head")),
        P(("seq", "head")),
        P(None, ("seq", "head")),
        P(("seq", "head")),
        P(("rep", "sub"), None, ("seq", "head")),
        P(("seq", "head"), None),
    )
    out_specs = (P(("rep", "sub"), "seq"), P(("rep", "sub"), None, ("seq", "head")))
    return jax.shard_map(local, mesh=mesh, in_specs=in_specs, out_specs=out_specs, check_vma=False)
```
